512 devices in a mesh: learner: 32 (over x, y), tensor: 16 (over z, core).
Axes of the slice: x: 4, y: 8, z: 8, core: 2. Of those that a mesh axis runs over, the one named last changes fastest.
Arguments:
- blocks: bfloat16 [256, 128, 4096], P('learner', None, 'tensor'), may hold values from -60 to 60
- seg_ids: int32 [32, 1024], P('learner'), may hold values from 0 to 7, never falling along the last dimension, each value on 1 to 256 neighbouring positions
- dest: int32 [256], replicated, may hold values from 0 to 31, as said below
- slot: int32 [256], replicated, may hold values from 0 to 7, as said below
- norm_gain: bfloat16 [4096], P('tensor'), may hold values from 0.25 to 1.75
- w_query: bfloat16 [4096, 4096], P(None, 'tensor'), may hold values from -2 to 2
- w_keyval: bfloat16 [4096, 2048], P('learner'), may hold values from -2 to 2
Outputs:
- context: bfloat16 [32768, 4096], P('learner', 'tensor')
The draws below stay inside these ranges and needn't reach their ends.
Inputs may be any that keep to these rules, and one draw needn't show every extreme that they name: `dest`: each learner receives exactly 8 blocks; at most 1 of the blocks of one learner go to any one learner, and in every draw some learner sends exactly 1 block to one learner. `slot`: the blocks that one learner receives take the positions 0 to 7 of its packed row, one each.
All inputs are finite; a program needn't handle non-finite values.
Results may differ from the reference program's by a relative error of at most 0.012.
The reference program's roundings to bfloat16 on the way (of `packed`, `normed`, `queries`, `keyval` and `probs`) count: a program that leaves them out, or rounds other values in their place, can miss the bound.
Values may be sent and summed in bfloat16 or wider, within the bound.
A program may use at most 64 MiB of HBM per device.

```python
import math
import jax
import jax.numpy as jnp
import numpy as np
from jax import lax

D = 4096
HEADS = 32
KV_HEADS = 8
HD = 128
BLOCK = 128
BLK_DEV = 8
PACK = 1024
TOKENS = 32768
N_LEARNER = 32


def routing_tables(key):
    base = jax.random.fold_in(key, 11)
    first_key, second_key, third_key = jax.random.split(base, 3)
    outer = jax.random.permutation(first_key, N_LEARNER).astype(jnp.int32)
    inner = jax.random.permutation(second_key, N_LEARNER).astype(jnp.int32)
    turns = jax.random.randint(third_key, (N_LEARNER,), 0, BLK_DEV).astype(jnp.int32)
    counter = jnp.arange(N_LEARNER * BLK_DEV, dtype=jnp.int32)
    source = counter // BLK_DEV
    within = counter % BLK_DEV
    targets = outer[(inner[source] + within) % N_LEARNER]
    places = (within + turns[targets]) % BLK_DEV
    return (targets.astype(jnp.int32), places.astype(jnp.int32))


def draw_dest(key, part):
    return routing_tables(key)[0]


def draw_slot(key, part):
    return routing_tables(key)[1]


def shared_weights(key):
    base = jax.random.fold_in(key, 7)
    query_key, keyval_key = jax.random.split(base, 2)
    w_query = jax.random.normal(query_key, (D, HEADS * HD), jnp.float32) / math.sqrt(D)
    w_keyval = jax.random.normal(keyval_key, (D, 2 * KV_HEADS * HD), jnp.float32) / math.sqrt(D)
    return (jnp.clip(w_query, -2.0, 2.0), jnp.clip(w_keyval, -2.0, 2.0))


def draw_w_query(key, part):
    return shared_weights(key)[0].astype(jnp.bfloat16)


def draw_w_keyval(key, part):
    return shared_weights(key)[1].astype(jnp.bfloat16)


def draw_blocks(key, part):
    base = jax.random.fold_in(key, 3)
    noise_key, scale_key = jax.random.split(base, 2)
    shape = (N_LEARNER * BLK_DEV, BLOCK, D)
    row_scale = jnp.exp(jax.random.uniform(scale_key, (N_LEARNER * BLK_DEV, BLOCK, 1), jnp.float32, 0.0, math.log(10.0)))
    values = jax.random.normal(noise_key, shape, jnp.float32) * row_scale
    return jnp.clip(values, -60.0, 60.0).astype(jnp.bfloat16)


def length_profile(count, total, limit, skew):
    weights = [(1 << 20) // math.isqrt(standing ** skew) + 1 for standing in range(2, count + 1)]
    spare, counts = total - limit - (count - 1), [1] * (count - 1)
    while spare > 0:
        movable = [i for i in range(count - 1) if counts[i] < limit]
        mass, left = sum([weights[i] for i in movable]), spare
        for i in movable:
            extra = min(limit - counts[i], max(1, left * weights[i] // mass), spare)
            counts[i] = counts[i] + extra
            spare = spare - extra
    return np.array([limit] + counts)


def ragged(rng, count, total, limit, lean):
    if count == 2:
        one = jax.random.randint(rng, (), max(1, total - limit), min(limit, total - 1) + 1)
        return jnp.stack([one, total - one])
    sizes = jnp.asarray(length_profile(count, total, limit, lean), jnp.int32)
    couples = (count - 1) // 2
    source_of, sink = sizes[1:1 + 2 * couples:2], sizes[2:2 + 2 * couples:2]
    room = jnp.minimum(source_of - 1, limit - sink)
    moved = jax.random.randint(jax.random.fold_in(rng, 1), (couples,), 0, 1 << 20) % (room + 1)
    sizes = sizes.at[1:1 + 2 * couples:2].set(source_of - moved).at[2:2 + 2 * couples:2].set(sink + moved)
    return sizes[jax.random.permutation(jax.random.fold_in(rng, 2), count)]


def setup_inputs(seed: int = 0) -> dict:
    key_list = jax.random.split(jax.random.key(seed), 8)
    blocks = draw_blocks(jax.random.fold_in(key_list[7], 71), 0)
    seg_ids = jax.vmap(lambda own: jnp.searchsorted(jnp.cumsum(ragged(own, 8, PACK, PACK // 4, 2)), jnp.arange(PACK), side="right"))(jax.random.split(key_list[1], N_LEARNER)).reshape((N_LEARNER, PACK)).astype(jnp.int32)
    dest = draw_dest(jax.random.fold_in(key_list[7], 71), 0)
    slot = draw_slot(jax.random.fold_in(key_list[7], 71), 0)
    norm_gain = jnp.clip(1.0 + 0.15 * jax.random.normal(key_list[4], (D,), jnp.float32), 0.25, 1.75).astype(jnp.bfloat16)
    w_query = draw_w_query(jax.random.fold_in(key_list[7], 71), 0)
    w_keyval = draw_w_keyval(jax.random.fold_in(key_list[7], 71), 0)
    return {"blocks": blocks, "seg_ids": seg_ids, "dest": dest, "slot": slot, "norm_gain": norm_gain, "w_query": w_query, "w_keyval": w_keyval}


def reference(blocks, seg_ids, dest, slot, norm_gain, w_query, w_keyval):
    positions = (dest * BLK_DEV + slot).astype(jnp.int32)
    packed = jnp.zeros_like(blocks).at[positions].set(blocks)
    packed = packed.reshape(N_LEARNER, BLK_DEV * BLOCK, D)
    group = HEADS // KV_HEADS

    def one_shard(shard_item):
        shard_rows, segment = shard_item
        widened = shard_rows.astype(jnp.float32)
        mean_sq = lax.optimization_barrier(jnp.mean(widened * widened, axis=-1, keepdims=True))
        normed = (widened * lax.rsqrt(mean_sq + 1e-05) * norm_gain.astype(jnp.float32)).astype(jnp.bfloat16)
        queries = jnp.dot(normed, w_query, preferred_element_type=jnp.float32).astype(jnp.bfloat16)
        keyval = jnp.dot(normed, w_keyval, preferred_element_type=jnp.float32).astype(jnp.bfloat16)
        length = shard_rows.shape[0]
        query_heads = queries.reshape(length, HEADS, HD).astype(jnp.float32)
        keyval_split = keyval.reshape(length, KV_HEADS, 2, HD).astype(jnp.float32)
        key_heads = jnp.repeat(keyval_split[:, :, 0], group, axis=1)
        value_heads = jnp.repeat(keyval_split[:, :, 1], group, axis=1)
        scores = jnp.einsum('qhd,khd->hqk', query_heads, key_heads) / math.sqrt(HD)
        index = jnp.arange(length, dtype=jnp.int32)
        allowed = (segment[:, None] == segment[None, :]) & (index[None, :] <= index[:, None])
        masked = jnp.where(allowed[None], scores, -1e+30)
        row_max = lax.optimization_barrier(jnp.max(masked, axis=-1, keepdims=True))
        exponent = jnp.where(allowed[None], jnp.exp(masked - row_max), 0.0)
        probs = (exponent / lax.optimization_barrier(jnp.sum(exponent, axis=-1, keepdims=True))).astype(jnp.bfloat16)
        context = jnp.einsum('hqk,khd->qhd', probs.astype(jnp.float32), value_heads)
        return context.astype(jnp.bfloat16).reshape(length, HEADS * HD)
    result = lax.map(one_shard, (packed, seg_ids))
    return result.reshape(TOKENS, HEADS * HD)
```

```python
import functools
import math

import jax
import jax.numpy as jnp
from jax import lax
from jax.experimental import pallas as pl
from jax.experimental.pallas import tpu as pltpu
from jax.sharding import PartitionSpec as P

D = 4096
HEADS = 32
KV_HEADS = 8
HD = 128
MESH = pl.DeviceIdType.MESH
F32 = jnp.float32
BF16 = jnp.bfloat16
TILES = 130
HALF = 65


def comm_kernel(
    inv, blocks, gain, wkv, xall, wout,
    gathered, sorted_, landed,
    local_sem, send_a, recv_a, send_b, recv_b,
    send_z, recv_z, send_d, recv_d,
    send_w, recv_wy, recv_wx, recv_wd,
):
    l = lax.axis_index("learner")
    t = lax.axis_index("tensor")
    x, y = lax.div(l, 8), lax.rem(l, 8)
    z, c = lax.div(t, 2), lax.rem(t, 2)
    other = z * 2 + (1 - c)

    def plane(j):
        return (j, t)

    def at_offset(i):
        return lax.rem(x + lax.div(i, 8), 4) * 8 + lax.rem(y + lax.rem(i, 8), 8)

    def peer(i, f):
        return lax.rem(x + lax.div(i, 4), 4) * 8 + lax.rem(lax.div(y, 2) + lax.rem(i, 4), 4) * 2 + f

    def place(j):
        return lax.div(j, 8) * 4 + lax.div(lax.rem(j, 8), 2)

    own_f = lax.rem(y, 2)
    own_place = place(l)

    barrier = pltpu.get_barrier_semaphore()

    def greet(i, carry):
        pl.semaphore_signal(barrier, inc=1, device_id=plane(at_offset(i)), device_id_type=MESH)
        return carry

    lax.fori_loop(1, 32, greet, 0)
    up = lax.rem(z + 1, 8) * 2 + c
    down = lax.rem(z + 7, 8) * 2 + c
    for who in (up, down, other):
        pl.semaphore_signal(barrier, inc=1, device_id=(l, who), device_id_type=MESH)
    pl.semaphore_wait(barrier, 34)

    def rows_of(j):
        return pl.ds(pl.multiple_of(j * 8, 8), 8)

    def piece_src(j, f):
        return blocks.at[:, pl.ds(pl.multiple_of(place(j) * 8, 8), 8), pl.ds(f * 128, 128)]

    for f in range(2):

        def send(i, carry, f=f):
            j = peer(i, f)

            @pl.when(j != l)
            def _():
                pltpu.make_async_remote_copy(
                    src_ref=piece_src(j, f),
                    dst_ref=gathered.at[rows_of(l)],
                    send_sem=send_a,
                    recv_sem=recv_a.at[l],
                    device_id=plane(j),
                    device_id_type=MESH,
                ).start()

            @pl.when(j == l)
            def _():
                pltpu.make_async_copy(piece_src(j, f), gathered.at[rows_of(l)], local_sem).start()

            return carry

        lax.fori_loop(0, 16, send, 0)

    pltpu.make_async_copy(gathered.at[rows_of(l)], gathered.at[rows_of(l)], local_sem).wait()

    def await_a(i, carry):
        j = at_offset(i)
        pltpu.make_async_copy(gathered.at[rows_of(j)], gathered.at[rows_of(j)], recv_a.at[j]).wait()
        return carry

    lax.fori_loop(1, 32, await_a, 0)

    def sort(j, carry):
        for s in range(8):
            sorted_[j * 8 + s] = gathered[inv[j * 8 + s]]
        return carry

    lax.fori_loop(0, 32, sort, 0)

    def send_out(i, carry):
        j = at_offset(i)
        pltpu.make_async_remote_copy(
            src_ref=sorted_.at[rows_of(j)],
            dst_ref=landed.at[own_f, :, own_place],
            send_sem=send_b,
            recv_sem=recv_b.at[l],
            device_id=plane(j),
            device_id_type=MESH,
        ).start()
        return carry

    lax.fori_loop(1, 32, send_out, 0)
    for s in range(8):
        landed[own_f, s, own_place] = sorted_[l * 8 + s]

    cols = pl.ds(pl.multiple_of(z * 256, 256), 256)
    half_rows = pl.ds(pl.multiple_of(c * 64, 64), 64)
    w_src = wkv.at[half_rows, cols]
    own_w = pltpu.make_async_copy(w_src, wout.at[l, half_rows], local_sem)
    own_w.start()

    def send_wy(i, carry):
        j = x * 8 + lax.rem(y + i, 8)
        pltpu.make_async_remote_copy(
            src_ref=w_src,
            dst_ref=wout.at[l, half_rows],
            send_sem=send_w.at[0],
            recv_sem=recv_wy.at[y],
            device_id=plane(j),
            device_id_type=MESH,
        ).start()
        return carry

    lax.fori_loop(1, 8, send_wy, 0)

    def arrive(f):
        def await_b(i, carry):
            j = peer(i, f)

            @pl.when(j != l)
            def _():
                ref = landed.at[f, :, place(j)]
                pltpu.make_async_copy(ref, ref, recv_b.at[j]).wait()

            return carry

        lax.fori_loop(0, 16, await_b, 0)

        g = gain[:, f * 128 : (f + 1) * 128].astype(F32).reshape(1, 1, 128)
        row = lax.broadcasted_iota(jnp.int32, (8, 128), 0)
        ones = jnp.ones((8, 128), BF16)

        def scale(s, total):
            xv = landed[f, s].astype(F32)
            xall[z, c, f, pl.ds(s * 16, 16)] = (xv * g).astype(BF16)
            sq = (xv * xv).reshape(128, 128)
            hi = sq.astype(BF16)
            lo = (sq - hi.astype(F32)).astype(BF16)
            dims = (((1,), (1,)), ((), ()))
            sums = lax.dot_general(ones, hi, dims, preferred_element_type=F32)
            sums += lax.dot_general(ones, lo, dims, preferred_element_type=F32)
            return jnp.where(row == s, sums, total)

        total = lax.fori_loop(0, 8, scale, jnp.zeros((8, 128), F32))
        hi = total.astype(BF16)
        xall[z, c, f, 128] = hi
        xall[z, c, f, 129] = (total - hi.astype(F32)).astype(BF16)

    def part(zo, cc, f, h):
        return xall.at[zo, cc, f, pl.ds(HALF * h, HALF)]

    def to_ring(zo, f, h, way, step):
        pltpu.make_async_remote_copy(
            src_ref=part(zo, c, f, h),
            dst_ref=part(zo, c, f, h),
            send_sem=send_z,
            recv_sem=recv_z.at[f, h, way, step],
            device_id=(l, up if way == 0 else down),
            device_id_type=MESH,
        ).start()

    def to_sibling(zo, f, h, k):
        pltpu.make_async_remote_copy(
            src_ref=part(zo, c, f, h),
            dst_ref=part(zo, c, f, h),
            send_sem=send_d,
            recv_sem=recv_d.at[f, h, k],
            device_id=(l, other),
            device_id_type=MESH,
        ).start()

    def begin(f):
        for h in range(2):
            to_ring(z, f, h, 0, 0)
            to_ring(z, f, h, 1, 0)
        for h in range(2):
            to_sibling(z, f, h, 0)

    def ring(f, step):
        for h in range(2):
            for way in range(2):
                if step == 4 and way != h:
                    continue
                k = (8 - step) if way == 0 else step
                zo = lax.rem(z + k, 8)
                ref = part(zo, c, f, h)
                pltpu.make_async_copy(ref, ref, recv_z.at[f, h, way, step - 1]).wait()
                if step < 3 or (step == 3 and way == h):
                    to_ring(zo, f, h, way, step)
                to_sibling(zo, f, h, k)

    def weights_x():
        own_w.wait()

        def await_wy(i, carry):
            yy = lax.rem(y + i, 8)
            ref = wout.at[x * 8 + yy, half_rows]
            pltpu.make_async_copy(ref, ref, recv_wy.at[yy]).wait()
            return carry

        lax.fori_loop(1, 8, await_wy, 0)
        for i in range(1, 4):
            mine = wout.at[pl.ds(pl.multiple_of(x * 8, 8), 8), half_rows]
            pltpu.make_async_remote_copy(
                src_ref=mine,
                dst_ref=mine,
                send_sem=send_w.at[1],
                recv_sem=recv_wx.at[x],
                device_id=plane(lax.rem(x + i, 4) * 8 + y),
                device_id_type=MESH,
            ).start()

    def weights_sibling():
        for i in range(1, 4):
            xx = lax.rem(x + i, 4)
            ref = wout.at[pl.ds(pl.multiple_of(xx * 8, 8), 8), half_rows]
            pltpu.make_async_copy(ref, ref, recv_wx.at[xx]).wait()
        pltpu.make_async_remote_copy(
            src_ref=wout.at[:, half_rows],
            dst_ref=wout.at[:, half_rows],
            send_sem=send_w.at[2],
            recv_sem=recv_wd,
            device_id=(l, other),
            device_id_type=MESH,
        ).start()

    arrive(0)
    begin(0)
    ring(0, 1)
    weights_x()
    ring(0, 2)
    arrive(1)
    begin(1)
    ring(0, 3)
    ring(1, 1)
    ring(0, 4)
    weights_sibling()
    ring(1, 2)
    ring(1, 3)
    ring(1, 4)

    for f in range(2):
        for h in range(2):
            for k in range(8):
                ref = part(lax.rem(z + k, 8), 1 - c, f, h)
                pltpu.make_async_copy(ref, ref, recv_d.at[f, h, k]).wait()
    their = wout.at[:, pl.ds(pl.multiple_of((1 - c) * 64, 64), 64)]
    pltpu.make_async_copy(their, their, recv_wd).wait()

    def drain(ref, sem):
        pltpu.make_async_copy(ref, ref, sem).wait()

    drain(gathered.at[pl.ds(0, 248)], send_a)
    drain(gathered.at[pl.ds(0, 248)], send_b)
    drain(xall.at[pl.ds(0, 7), :, 0], send_z)
    drain(xall.at[:, :, 0], send_d)
    drain(wout.at[pl.ds(0, 7), half_rows], send_w.at[0])
    drain(wout.at[pl.ds(0, 24), half_rows], send_w.at[1])
    drain(wout.at[:, half_rows], send_w.at[2])


def compute_kernel(xt, sums, wq, wk, seg, out, keys, values, rms, segc):
    i = pl.program_id(0)

    @pl.when(i == 0)
    def _():
        keys[0:256] = jnp.zeros((256, HD), BF16)
        values[0:256] = jnp.zeros((256, HD), BF16)
        total = jnp.zeros((8, 128), F32)
        for zz in range(8):
            for cc in range(2):
                for f in range(2):
                    both = sums[zz, cc, f].astype(F32)
                    total += both[0:8] + both[8:16]
        inverse = lax.rsqrt(total / D + 1e-05).T
        doc = seg[8:16].astype(F32).T
        for r in range(8):
            rms[r] = jnp.broadcast_to(inverse[:, r : r + 1], (128, 128))
            segc[r] = jnp.broadcast_to(doc[:, r : r + 1], (128, 128))

    acc = jnp.zeros((256, 512), F32)
    for zz in range(8):
        for f in range(2):
            xs = jnp.concatenate([xt[zz, 0, f], xt[zz, 1, f]], axis=1)
            lo, hi = (zz * 2) * 256 + f * 128, (zz * 2 + 1) * 256 + f * 128
            top = jnp.concatenate([wq[lo : lo + 128], wk[zz * 4 + f]], axis=1)
            bottom = jnp.concatenate([wq[hi : hi + 128], wk[zz * 4 + 2 + f]], axis=1)
            acc += jnp.dot(xs, jnp.concatenate([top, bottom], axis=0), preferred_element_type=F32)
    r2 = jnp.concatenate([rms[2 * i], rms[2 * i + 1]], axis=0)[:, 0:1]
    acc = acc * r2
    q = acc[:, 0:256].astype(BF16)
    start = pl.multiple_of(i * 256, 256)
    keys[pl.ds(start + 256, 256)] = acc[:, 256:384].astype(BF16)
    values[pl.ds(start + 256, 256)] = acc[:, 384:512].astype(BF16)
    kw = keys[pl.ds(start, 512)]
    vw = values[pl.ds(start, 512)]
    qdoc = jnp.concatenate([segc[2 * i], segc[2 * i + 1]], axis=0)[:, 0:1]
    kdoc = jnp.concatenate([seg[pl.ds(6 + 2 * i + n, 1)] for n in range(4)], axis=1).astype(F32)
    row = lax.broadcasted_iota(jnp.int32, (256, 512), 0)
    col = lax.broadcasted_iota(jnp.int32, (256, 512), 1)
    allowed = (qdoc == kdoc) & (col <= row + 256)
    for h in range(2):
        s = lax.dot_general(
            q[:, h * HD : (h + 1) * HD], kw, (((1,), (1,)), ((), ())), preferred_element_type=F32
        )
        masked = jnp.where(allowed, s * (1.0 / math.sqrt(HD)), -1e30)
        top = jnp.max(masked, axis=-1, keepdims=True)
        e = jnp.where(allowed, jnp.exp(masked - top), 0.0)
        p = (e * (1.0 / jnp.sum(e, axis=-1, keepdims=True))).astype(BF16)
        out[:, h * HD : (h + 1) * HD] = jnp.dot(p, vw, preferred_element_type=F32).astype(BF16)


def on_device(blocks, seg_ids, dest, slot, norm_gain, w_query, w_keyval):
    ids = jnp.arange(256, dtype=jnp.int32)
    position = dest * 8 + slot
    inv = jnp.sum(jnp.where(position[None, :] == ids[:, None], ids[None, :], 0), axis=1)
    dma = pltpu.SemaphoreType.DMA
    anywhere = pl.BlockSpec(memory_space=pl.ANY)
    vmem = pl.BlockSpec(memory_space=pltpu.VMEM)
    xall, wk = pl.pallas_call(
        comm_kernel,
        out_shape=(
            jax.ShapeDtypeStruct((8, 2, 2, TILES, 8, 128), BF16),
            jax.ShapeDtypeStruct((32, 128, 256), BF16),
        ),
        in_specs=[pl.BlockSpec(memory_space=pltpu.SMEM), anywhere, vmem, anywhere],
        out_specs=(vmem, vmem),
        scratch_shapes=[
            pltpu.VMEM((256, 8, 128), BF16),
            pltpu.VMEM((256, 8, 128), BF16),
            pltpu.VMEM((2, 8, 16, 8, 128), BF16),
            dma, dma, dma((32,)), dma, dma((32,)),
            dma, dma((2, 2, 2, 4)), dma, dma((2, 2, 8)),
            dma((3,)), dma((8,)), dma((4,)), dma,
        ],
        compiler_params=pltpu.CompilerParams(
            collective_id=0, has_side_effects=True, vmem_limit_bytes=40 * 1024 * 1024
        ),
        name="exchange",
    )(inv.astype(jnp.int32), blocks, norm_gain.reshape(1, 256), w_keyval)
    xall = xall.reshape(8, 2, 2, TILES * 8, 128)
    rows = seg_ids.reshape(8, 128)
    seg = jnp.concatenate([jnp.full((8, 128), -1, jnp.int32), rows], axis=0)
    return pl.pallas_call(
        compute_kernel,
        grid=(4,),
        out_shape=jax.ShapeDtypeStruct((1024, 256), BF16),
        in_specs=[
            pl.BlockSpec((8, 2, 2, 256, 128), lambda i: (0, 0, 0, i, 0)),
            pl.BlockSpec((8, 2, 2, 16, 128), lambda i: (0, 0, 0, 64, 0)),
            pl.BlockSpec((4096, 256), lambda i: (0, 0)),
            pl.BlockSpec((32, 128, 256), lambda i: (0, 0, 0)),
            pl.BlockSpec((16, 128), lambda i: (0, 0)),
        ],
        out_specs=pl.BlockSpec((256, 256), lambda i: (i, 0)),
        scratch_shapes=[
            pltpu.VMEM((1280, HD), BF16),
            pltpu.VMEM((1280, HD), BF16),
            pltpu.VMEM((8, 128, 128), F32),
            pltpu.VMEM((8, 128, 128), F32),
        ],
        compiler_params=pltpu.CompilerParams(
            dimension_semantics=("arbitrary",), vmem_limit_bytes=40 * 1024 * 1024
        ),
        name="project_attend",
    )(xall, xall, w_query, wk, seg)


def solution(mesh):
    return jax.shard_map(
        on_device,
        mesh=mesh,
        in_specs=(
            P("learner", None, "tensor"),
            P("learner", None),
            P(),
            P(),
            P("tensor"),
            P(None, "tensor"),
            P("learner", None),
        ),
        out_specs=P("learner", "tensor"),
        check_vma=False,
    )
```

```python
import math

import jax
import jax.numpy as jnp
from jax import lax
from jax.experimental import pallas as pl
from jax.experimental.pallas import tpu as pltpu
from jax.sharding import PartitionSpec as P

D = 4096
HD = 128
MESH = pl.DeviceIdType.MESH
F32 = jnp.float32
BF16 = jnp.bfloat16
I32 = jnp.int32
ROWS = 528


def exchange_kernel(
    dest, slot, blocks, gain, wkv, wq, out,
    own, gathered, sorted_, landed, xall, wk, wq_v, acc, ready, inv_v, inv,
    own_sem, wq_sem, inv_sem, out_sem, w_sem,
    send_a, recv_a, send_b, recv_b, send_z, recv_z, send_d, recv_d,
    send_w, recv_wy, recv_wx, recv_wd,
):
    l = lax.axis_index("learner")
    t = lax.axis_index("tensor")
    x, y = lax.div(l, 8), lax.rem(l, 8)
    z, c = lax.div(t, 2), lax.rem(t, 2)
    other = z * 2 + (1 - c)
    up = lax.rem(z + 1, 8) * 2 + c
    down = lax.rem(z + 7, 8) * 2 + c

    def at_offset(i):
        return lax.rem(x + lax.div(i, 8), 4) * 8 + lax.rem(y + lax.rem(i, 8), 8)

    def peer(i, q):
        return lax.rem(x + lax.div(i, 2), 4) * 8 + lax.rem(lax.div(y, 4) + lax.rem(i, 2), 2) * 4 + q

    def place(j):
        return lax.div(j, 8) * 2 + lax.div(lax.rem(j, 8), 4)

    def pending(ref, sem):
        return pltpu.make_async_copy(ref, ref, sem)

    own_q = lax.rem(y, 4)
    own_place = place(l)

    barrier = pltpu.get_barrier_semaphore()

    def greet(i, carry):
        pl.semaphore_signal(barrier, inc=1, device_id=(at_offset(i), t), device_id_type=MESH)
        return carry

    lax.fori_loop(1, 32, greet, 0)
    for who in (up, down, other):
        pl.semaphore_signal(barrier, inc=1, device_id=(l, who), device_id_type=MESH)

    take_own = pltpu.make_async_copy(blocks, own, own_sem)
    take_own.start()
    take_wq = pltpu.make_async_copy(wq, wq_v, wq_sem)
    take_wq.start()
    position = dest[...] * 8 + slot[...]
    column = jnp.concatenate([position] * 4, axis=0).T
    where_to = lax.broadcasted_iota(I32, (128, 256), 1)
    who_from = lax.broadcasted_iota(I32, (128, 256), 0)
    table = jnp.zeros((1, 256), I32)
    for k in range(2):
        hit = column[:, k : k + 1] == where_to
        found = jnp.max(jnp.where(hit, who_from + 128 * k, 0), axis=0, keepdims=True)
        table = jnp.maximum(table, found)
    inv_v[...] = table
    take_inv = pltpu.make_async_copy(inv_v, inv, inv_sem)
    take_inv.start()
    take_own.wait()
    pl.semaphore_wait(barrier, 34)

    def rows_of(j):
        return pl.ds(pl.multiple_of(j * 8, 8), 8)

    for q in range(4):

        def send(i, carry, q=q):
            j = peer(i, q)
            src = own.at[:, 8 * (q % 2) + place(j), :, pl.ds((q // 2) * 128, 128)]

            @pl.when(j != l)
            def _():
                pltpu.make_async_remote_copy(
                    src_ref=src,
                    dst_ref=gathered.at[rows_of(l)],
                    send_sem=send_a,
                    recv_sem=recv_a.at[l],
                    device_id=(j, t),
                    device_id_type=MESH,
                ).start()

            @pl.when(j == l)
            def _():
                for b in range(8):
                    gathered[l * 8 + b] = own[b, 8 * (q % 2) + place(j), :, (q // 2) * 128 : (q // 2) * 128 + 128]

            return carry

        lax.fori_loop(0, 8, send, 0)

    take_inv.wait()

    def await_a(i, carry):
        j = at_offset(i)
        pending(gathered.at[rows_of(j)], recv_a.at[j]).wait()
        return carry

    lax.fori_loop(1, 32, await_a, 0)

    def sort(j, carry):
        for s in range(8):
            sorted_[j * 8 + s] = gathered[inv[0, j * 8 + s]]
        return carry

    lax.fori_loop(0, 32, sort, 0)

    def send_out(i, carry):
        j = at_offset(i)
        pltpu.make_async_remote_copy(
            src_ref=sorted_.at[rows_of(j)],
            dst_ref=landed.at[own_q, :, own_place],
            send_sem=send_b,
            recv_sem=recv_b.at[l],
            device_id=(j, t),
            device_id_type=MESH,
        ).start()
        return carry

    lax.fori_loop(1, 32, send_out, 0)
    for s in range(8):
        landed[own_q, s, own_place] = sorted_[l * 8 + s]

    half_rows = pl.ds(pl.multiple_of(c * 64, 64), 64)
    w_src = wkv.at[half_rows, pl.ds(pl.multiple_of(z * 256, 256), 256)]
    take_w = pltpu.make_async_copy(w_src, wk.at[l, half_rows], w_sem)
    take_w.start()

    def send_wy(i, carry):
        pltpu.make_async_remote_copy(
            src_ref=w_src,
            dst_ref=wk.at[l, half_rows],
            send_sem=send_w.at[0],
            recv_sem=recv_wy.at[y],
            device_id=(x * 8 + lax.rem(y + i, 8), t),
            device_id_type=MESH,
        ).start()
        return carry

    lax.fori_loop(1, 8, send_wy, 0)

    def weights_x():
        take_w.wait()

        def await_wy(i, carry):
            yy = lax.rem(y + i, 8)
            pending(wk.at[x * 8 + yy, half_rows], recv_wy.at[yy]).wait()
            return carry

        lax.fori_loop(1, 8, await_wy, 0)
        for way in range(2):
            to_column(x, 8, 0, way)

    def column(xx, first, count):
        return wk.at[pl.ds(pl.multiple_of(xx * 8 + first, 4), count), half_rows]

    def to_column(xx, count, first, way):
        ref = column(xx, first, count)
        pltpu.make_async_remote_copy(
            src_ref=ref,
            dst_ref=ref,
            send_sem=send_w.at[1],
            recv_sem=recv_wx.at[way, 0 if count == 8 else 1],
            device_id=(lax.rem(x + (1 if way == 0 else 3), 4) * 8 + y, t),
            device_id_type=MESH,
        ).start()

    def weights_x2():
        for way in range(2):
            xx = lax.rem(x + (3 if way == 0 else 1), 4)
            pending(column(xx, 0, 8), recv_wx.at[way, 0]).wait()
            to_column(xx, 4, 4 * way, way)

    def weights_sibling():
        xx = lax.rem(x + 2, 4)
        for way in range(2):
            pending(column(xx, 4 * way, 4), recv_wx.at[way, 1]).wait()
        mine = wk.at[:, half_rows]
        pltpu.make_async_remote_copy(
            src_ref=mine,
            dst_ref=mine,
            send_sem=send_w.at[2],
            recv_sem=recv_wd,
            device_id=(l, other),
            device_id_type=MESH,
        ).start()

    def weights_ready():
        pending(wk.at[:, pl.ds(pl.multiple_of((1 - c) * 64, 64), 64)], recv_wd).wait()

    row = lax.broadcasted_iota(I32, (8, 128), 0)

    def arrive(q):
        def await_b(i, carry):
            j = peer(i, q)

            @pl.when(j != l)
            def _():
                pending(landed.at[q, :, place(j)], recv_b.at[j]).wait()

            return carry

        lax.fori_loop(0, 8, await_b, 0)
        f = q // 2
        g = gain[f * 128 : (f + 1) * 128].astype(F32).reshape(1, 128)
        ones = jnp.ones((8, 128), BF16)
        dims = (((1,), (1,)), ((), ()))

        def scale(j, total):
            xv = landed[q, pl.ds(2 * j, 2)].astype(F32).reshape(128, 128)
            xall[z, c, q, pl.ds(pl.multiple_of(j * 128, 128), 128)] = (xv * g).astype(BF16)
            sq = xv * xv
            hi = sq.astype(BF16)
            lo = (sq - hi.astype(F32)).astype(BF16)
            sums = lax.dot_general(ones, hi, dims, preferred_element_type=F32)
            sums += lax.dot_general(ones, lo, dims, preferred_element_type=F32)
            return jnp.where(lax.rem(row, 4) == j, sums, total)

        total = lax.fori_loop(0, 4, scale, jnp.zeros((8, 128), F32))
        hi = total.astype(BF16).astype(F32)
        tile = jnp.where(row < 4, hi, total - hi)
        xall[z, c, q, 512:528] = jnp.concatenate([tile, jnp.zeros((8, 128), F32)], axis=0).astype(BF16)

    def to_ring(zo, q, way, step):
        pltpu.make_async_remote_copy(
            src_ref=xall.at[zo, c, q],
            dst_ref=xall.at[zo, c, q],
            send_sem=send_z,
            recv_sem=recv_z.at[q, way, step],
            device_id=(l, up if way == 0 else down),
            device_id_type=MESH,
        ).start()

    def to_sibling(zo, q, k):
        pltpu.make_async_remote_copy(
            src_ref=xall.at[zo, c, q],
            dst_ref=xall.at[zo, c, q],
            send_sem=send_d,
            recv_sem=recv_d.at[q, k],
            device_id=(l, other),
            device_id_type=MESH,
        ).start()

    def begin(q):
        to_ring(z, q, 0, 0)
        to_ring(z, q, 1, 0)
        to_sibling(z, q, 0)

    def ring(q, step):
        for way in range(2):
            if step == 4 and way != q % 2:
                continue
            k = (8 - step) if way == 0 else step
            zo = lax.rem(z + k, 8)
            pending(xall.at[zo, c, q], recv_z.at[q, way, step - 1]).wait()
            if step < 3 or (step == 3 and way == q % 2):
                to_ring(zo, q, way, step)
            to_sibling(zo, q, k)

    def project(kind, q, first, second):
        f, half = q // 2, q % 2
        zs = [lax.rem(z + k, 8) for k in (first, second)]
        if kind == 0:
            for k, zo in zip((first, second), zs):
                pending(xall.at[zo, 1 - c, q], recv_d.at[q, k]).wait()

        def some_rows(i, carry):
            start = pl.multiple_of(i * 256, 256)
            pairs = [(zo, cc) for zo in zs for cc in range(2)]
            lhs = jnp.concatenate([xall[zo, cc, q, pl.ds(start, 256)] for zo, cc in pairs], axis=1)
            if kind == 0:
                rhs = [wq_v[pl.ds(pl.multiple_of(zo * 512 + cc * 256 + f * 128, 128), 128)] for zo, cc in pairs]
            else:
                rhs = [wk[zo * 4 + cc * 2 + f] for zo, cc in pairs]
            got = jnp.dot(lhs, jnp.concatenate(rhs, axis=0), preferred_element_type=F32)
            at = pl.ds(pl.multiple_of(half * 512 + start, 256), 256)
            if f == 0 and first == 1:
                acc[kind, at] = got
            else:
                acc[kind, at] += got
            return carry

        lax.fori_loop(0, 2, some_rows, 0)

    for q in range(4):
        arrive(q)
        begin(q)
    weights_x()
    for q in range(4):
        ring(q, 1)
    weights_x2()
    take_wq.wait()
    for q in range(4):
        ring(q, 2)
        project(0, q, 1, 7)
    weights_sibling()
    for q in range(4):
        ring(q, 3)
        project(0, q, 2, 6)
    weights_ready()
    project(1, 0, 1, 7)
    project(1, 1, 1, 7)
    project(1, 2, 1, 7)
    ring(0, 4)
    project(1, 3, 1, 7)
    project(1, 0, 2, 6)
    project(1, 1, 2, 6)
    project(0, 0, 3, 5)
    project(1, 0, 3, 5)
    ring(1, 4)
    project(1, 2, 2, 6)
    project(1, 3, 2, 6)
    project(0, 1, 3, 5)
    project(1, 1, 3, 5)
    project(0, 2, 3, 5)
    ring(2, 4)
    project(1, 2, 3, 5)
    project(0, 3, 3, 5)
    project(1, 3, 3, 5)
    project(0, 0, 0, 4)
    ring(3, 4)
    project(1, 0, 0, 4)
    for q in range(1, 4):
        project(0, q, 0, 4)
        project(1, q, 0, 4)

    sums = []
    for half in range(2):
        total = jnp.zeros((8, 128), F32)
        for zz in range(8):
            for cc in range(2):
                for f in range(2):
                    total += xall[zz, cc, 2 * f + half, 512:528].astype(F32)[0:8]
        sums.append(total[0:4] + total[4:8])
    inverse = lax.rsqrt(jnp.concatenate(sums, axis=0) / D + 1e-05).T
    results = []
    for j in range(4):
        for half in range(2):
            start = half * 512 + j * 128
            factor = inverse[:, half * 4 + j : half * 4 + j + 1]
            for kind in range(2):
                scaled = (acc[kind, start : start + 128] * factor).astype(BF16)
                for e in range(2):
                    to = (2 * j + e) * 128 + half * 64
                    ready[to : to + 64, kind * 256 : kind * 256 + 256] = scaled[e * 64 : e * 64 + 64]
        at = pl.ds(256 * j, 256)
        result = pltpu.make_async_copy(ready.at[at], out.at[at], out_sem.at[j])
        result.start()
        results.append(result)

    pending(gathered.at[pl.ds(0, 248)], send_a).wait()
    pending(gathered.at[pl.ds(0, 248)], send_b).wait()
    pending(xall.at[pl.ds(0, 7), 0], send_z).wait()
    pending(xall.at[:, 0], send_d).wait()
    pending(wk.at[pl.ds(0, 7), half_rows], send_w.at[0]).wait()
    pending(wk.at[pl.ds(0, 24), half_rows], send_w.at[1]).wait()
    pending(wk.at[:, half_rows], send_w.at[2]).wait()
    for result in results:
        result.wait()


def attend_kernel(qkv, seg, out, held, buf, take_sem, sems):
    takes = []
    for i in range(4):
        at = pl.ds(256 * i, 256)
        take = pltpu.make_async_copy(qkv.at[at], held.at[at], take_sem.at[i])
        take.start()
        takes.append(take)
    docs = seg[...].astype(F32)
    columns = jnp.concatenate([docs[:, r * 128 : r * 128 + 128] for r in range(8)], axis=0).T
    copies = []
    for i in range(4):
        start, begin = 256 * i, max(0, 256 * i - 256)
        width = start + 256 - begin
        qdoc = jnp.concatenate([columns[:, 2 * i : 2 * i + 1], columns[:, 2 * i + 1 : 2 * i + 2]], axis=0)
        row = lax.broadcasted_iota(I32, (256, width), 0)
        col = lax.broadcasted_iota(I32, (256, width), 1)
        allowed = (qdoc == docs[:, begin : begin + width]) & (col <= row + (start - begin))
        takes[i].wait()
        keys = held[begin : begin + width, 2 * HD : 3 * HD]
        values = held[begin : begin + width, 3 * HD : 4 * HD]
        for h in range(2):
            s = lax.dot_general(
                held[start : start + 256, h * HD : (h + 1) * HD], keys, (((1,), (1,)), ((), ())),
                preferred_element_type=F32,
            )
            masked = jnp.where(allowed, s, -1e30)
            top = jnp.max(masked, axis=-1, keepdims=True)
            e = jnp.exp2((masked - top) * (math.log2(math.e) / math.sqrt(HD)))
            part = jnp.dot(e.astype(BF16), values, preferred_element_type=F32)
            part = part * (1.0 / jnp.sum(e, axis=-1, keepdims=True))
            buf[start : start + 256, h * HD : (h + 1) * HD] = part.astype(BF16)
        at = pl.ds(start, 256)
        copy = pltpu.make_async_copy(buf.at[at], out.at[at], sems.at[i])
        copy.start()
        copies.append(copy)
    for copy in copies:
        copy.wait()


def on_device(blocks, seg_ids, dest, slot, norm_gain, w_query, w_keyval):
    dma = pltpu.SemaphoreType.DMA
    hbm = pl.BlockSpec(memory_space=pltpu.HBM)
    vmem = pl.BlockSpec(memory_space=pltpu.VMEM)
    qkv = pl.pallas_call(
        exchange_kernel,
        out_shape=jax.ShapeDtypeStruct((1024, 512), BF16),
        in_specs=[vmem, vmem, hbm, vmem, hbm, hbm],
        out_specs=hbm,
        scratch_shapes=[
            pltpu.VMEM((8, 16, 8, 256), BF16),
            pltpu.VMEM((256, 8, 128), BF16),
            pltpu.VMEM((256, 8, 128), BF16),
            pltpu.VMEM((4, 8, 8, 8, 128), BF16),
            pltpu.VMEM((8, 2, 4, ROWS, 128), BF16),
            pltpu.VMEM((32, 128, 256), BF16),
            pltpu.VMEM((4096, 256), BF16),
            pltpu.VMEM((2, 1024, 256), F32),
            pltpu.VMEM((1024, 512), BF16),
            pltpu.VMEM((1, 256), I32),
            pltpu.SMEM((1, 256), I32),
            dma, dma, dma, dma((4,)), dma,
            dma, dma((32,)), dma, dma((32,)), dma, dma((4, 2, 4)), dma, dma((4, 8)),
            dma((3,)), dma((8,)), dma((2, 2)), dma,
        ],
        compiler_params=pltpu.CompilerParams(
            collective_id=0, has_side_effects=True, vmem_limit_bytes=60 * 1024 * 1024
        ),
        name="exchange",
    )(
        dest.reshape(2, 128),
        slot.reshape(2, 128),
        blocks.reshape(8, 16, 8, 256),
        norm_gain,
        w_keyval,
        w_query,
    )
    return pl.pallas_call(
        attend_kernel,
        out_shape=jax.ShapeDtypeStruct((1024, 256), BF16),
        in_specs=[hbm, vmem],
        out_specs=hbm,
        scratch_shapes=[pltpu.VMEM((1024, 512), BF16), pltpu.VMEM((1024, 256), BF16), dma((4,)), dma((4,))],
        compiler_params=pltpu.CompilerParams(vmem_limit_bytes=60 * 1024 * 1024),
        name="attend",
    )(qkv, seg_ids)


def solution(mesh):
    return jax.shard_map(
        on_device,
        mesh=mesh,
        in_specs=(
            P("learner", None, "tensor"),
            P("learner", None),
            P(),
            P(),
            P("tensor"),
            P(None, "tensor"),
            P("learner", None),
        ),
        out_specs=P("learner", "tensor"),
        check_vma=False,
    )
```

```python
import math

import jax
import jax.numpy as jnp
from jax import lax
from jax.experimental import pallas as pl
from jax.experimental.pallas import tpu as pltpu
from jax.sharding import PartitionSpec as P

D = 4096
HD = 128
MESH = pl.DeviceIdType.MESH
F32 = jnp.float32
BF16 = jnp.bfloat16
I32 = jnp.int32
ROWS = 528


def exchange_kernel(
    dest, slot, blocks, gain, wkv, wq, out,
    own, gathered, sorted_, landed, xall, wk, wq_v, acc, ready, inv_v, inv,
    own_sem, wq_sem, inv_sem, out_sem, w_sem,
    send_a, recv_a, send_b, recv_b, send_z, recv_z, send_d, recv_d,
    send_w, recv_wy, recv_wx, recv_wd,
):
    l = lax.axis_index("learner")
    t = lax.axis_index("tensor")
    x, y = lax.div(l, 8), lax.rem(l, 8)
    z, c = lax.div(t, 2), lax.rem(t, 2)
    other = z * 2 + (1 - c)
    up = lax.rem(z + 1, 8) * 2 + c
    down = lax.rem(z + 7, 8) * 2 + c

    def at_offset(i):
        return lax.rem(x + lax.div(i, 8), 4) * 8 + lax.rem(y + lax.rem(i, 8), 8)

    def peer(i, q):
        return lax.rem(x + lax.div(i, 2), 4) * 8 + lax.rem(lax.div(y, 4) + lax.rem(i, 2), 2) * 4 + q

    def place(j):
        return lax.div(j, 8) * 2 + lax.div(lax.rem(j, 8), 4)

    def pending(ref, sem):
        return pltpu.make_async_copy(ref, ref, sem)

    own_q = lax.rem(y, 4)
    own_place = place(l)

    barrier = pltpu.get_barrier_semaphore()

    def greet(i, carry):
        pl.semaphore_signal(barrier, inc=1, device_id=(at_offset(i), t), device_id_type=MESH)
        return carry

    lax.fori_loop(1, 32, greet, 0)
    for who in (up, down, other):
        pl.semaphore_signal(barrier, inc=1, device_id=(l, who), device_id_type=MESH)

    take_own = pltpu.make_async_copy(blocks, own, own_sem)
    take_own.start()
    take_wq = pltpu.make_async_copy(wq, wq_v, wq_sem)
    take_wq.start()
    position = dest[...] * 8 + slot[...]
    column = jnp.concatenate([position] * 4, axis=0).T
    where_to = lax.broadcasted_iota(I32, (128, 256), 1)
    who_from = lax.broadcasted_iota(I32, (128, 256), 0)
    table = jnp.zeros((1, 256), I32)
    for k in range(2):
        hit = column[:, k : k + 1] == where_to
        found = jnp.max(jnp.where(hit, who_from + 128 * k, 0), axis=0, keepdims=True)
        table = jnp.maximum(table, found)
    inv_v[...] = table
    take_inv = pltpu.make_async_copy(inv_v, inv, inv_sem)
    take_inv.start()
    take_own.wait()
    pl.semaphore_wait(barrier, 34)

    def rows_of(j):
        return pl.ds(pl.multiple_of(j * 8, 8), 8)

    def scatter(q):
        def send(i, carry):
            j = peer(i, q)
            src = own.at[:, 8 * (q % 2) + place(j), :, pl.ds((q // 2) * 128, 128)]

            @pl.when(j != l)
            def _():
                pltpu.make_async_remote_copy(
                    src_ref=src,
                    dst_ref=gathered.at[rows_of(l)],
                    send_sem=send_a,
                    recv_sem=recv_a.at[l],
                    device_id=(j, t),
                    device_id_type=MESH,
                ).start()

            @pl.when(j == l)
            def _():
                for b in range(8):
                    gathered[l * 8 + b] = own[b, 8 * (q % 2) + place(j), :, (q // 2) * 128 : (q // 2) * 128 + 128]

            return carry

        lax.fori_loop(0, 8, send, 0)

    scatter(0)
    scatter(1)
    scatter(2)
    scatter(3)
    take_inv.wait()

    def await_a(i, carry):
        j = at_offset(i)
        pending(gathered.at[rows_of(j)], recv_a.at[j]).wait()
        return carry

    def sort(j, carry):
        for s in range(8):
            sorted_[j * 8 + s] = gathered[inv[0, j * 8 + s]]
        return carry

    def send_out(i, carry):
        j = at_offset(i)
        pltpu.make_async_remote_copy(
            src_ref=sorted_.at[rows_of(j)],
            dst_ref=landed.at[own_q, :, own_place],
            send_sem=send_b,
            recv_sem=recv_b.at[l],
            device_id=(j, t),
            device_id_type=MESH,
        ).start()
        return carry

    def distribute():
        lax.fori_loop(1, 32, await_a, 0)
        lax.fori_loop(0, 32, sort, 0)
        lax.fori_loop(1, 32, send_out, 0)
        for s in range(8):
            landed[own_q, s, own_place] = sorted_[l * 8 + s]

    half_rows = pl.ds(pl.multiple_of(c * 64, 64), 64)
    w_src = wkv.at[half_rows, pl.ds(pl.multiple_of(z * 256, 256), 256)]
    take_w = pltpu.make_async_copy(w_src, wk.at[l, half_rows], w_sem)
    take_w.start()

    def send_wy(i, carry):
        pltpu.make_async_remote_copy(
            src_ref=w_src,
            dst_ref=wk.at[l, half_rows],
            send_sem=send_w.at[0],
            recv_sem=recv_wy.at[y],
            device_id=(x * 8 + lax.rem(y + i, 8), t),
            device_id_type=MESH,
        ).start()
        return carry

    def weights_x():
        take_w.wait()

        def await_wy(i, carry):
            yy = lax.rem(y + i, 8)
            pending(wk.at[x * 8 + yy, half_rows], recv_wy.at[yy]).wait()
            return carry

        lax.fori_loop(1, 8, await_wy, 0)
        for way in range(2):
            to_column(x, 8, 0, way)

    def column(xx, first, count):
        return wk.at[pl.ds(pl.multiple_of(xx * 8 + first, 4), count), half_rows]

    def to_column(xx, count, first, way):
        ref = column(xx, first, count)
        pltpu.make_async_remote_copy(
            src_ref=ref,
            dst_ref=ref,
            send_sem=send_w.at[1],
            recv_sem=recv_wx.at[way, 0 if count == 8 else 1],
            device_id=(lax.rem(x + (1 if way == 0 else 3), 4) * 8 + y, t),
            device_id_type=MESH,
        ).start()

    def weights_x2():
        for way in range(2):
            xx = lax.rem(x + (3 if way == 0 else 1), 4)
            pending(column(xx, 0, 8), recv_wx.at[way, 0]).wait()
            to_column(xx, 4, 4 * way, way)

    def weights_sibling():
        xx = lax.rem(x + 2, 4)
        for way in range(2):
            pending(column(xx, 4 * way, 4), recv_wx.at[way, 1]).wait()
        mine = wk.at[:, half_rows]
        pltpu.make_async_remote_copy(
            src_ref=mine,
            dst_ref=mine,
            send_sem=send_w.at[2],
            recv_sem=recv_wd,
            device_id=(l, other),
            device_id_type=MESH,
        ).start()

    def weights_ready():
        pending(wk.at[:, pl.ds(pl.multiple_of((1 - c) * 64, 64), 64)], recv_wd).wait()

    row = lax.broadcasted_iota(I32, (8, 128), 0)

    def arrive(q):
        def await_b(i, carry):
            j = peer(i, q)

            @pl.when(j != l)
            def _():
                pending(landed.at[q, :, place(j)], recv_b.at[j]).wait()

            return carry

        lax.fori_loop(0, 8, await_b, 0)
        f = q // 2
        g = gain[f * 128 : (f + 1) * 128].astype(F32).reshape(1, 128)
        ones = jnp.ones((8, 128), BF16)
        dims = (((1,), (1,)), ((), ()))

        def scale(j, total):
            xv = landed[q, pl.ds(2 * j, 2)].astype(F32).reshape(128, 128)
            xall[z, c, q, pl.ds(pl.multiple_of(j * 128, 128), 128)] = (xv * g).astype(BF16)
            sq = xv * xv
            hi = sq.astype(BF16)
            lo = (sq - hi.astype(F32)).astype(BF16)
            sums = lax.dot_general(ones, hi, dims, preferred_element_type=F32)
            sums += lax.dot_general(ones, lo, dims, preferred_element_type=F32)
            return jnp.where(lax.rem(row, 4) == j, sums, total)

        total = lax.fori_loop(0, 4, scale, jnp.zeros((8, 128), F32))
        hi = total.astype(BF16).astype(F32)
        tile = jnp.where(row < 4, hi, total - hi)
        xall[z, c, q, 512:528] = jnp.concatenate([tile, jnp.zeros((8, 128), F32)], axis=0).astype(BF16)

    def to_ring(zo, q, way, step):
        pltpu.make_async_remote_copy(
            src_ref=xall.at[zo, c, q],
            dst_ref=xall.at[zo, c, q],
            send_sem=send_z,
            recv_sem=recv_z.at[q, way, step],
            device_id=(l, up if way == 0 else down),
            device_id_type=MESH,
        ).start()

    def to_sibling(zo, q, k):
        pltpu.make_async_remote_copy(
            src_ref=xall.at[zo, c, q],
            dst_ref=xall.at[zo, c, q],
            send_sem=send_d,
            recv_sem=recv_d.at[q, k],
            device_id=(l, other),
            device_id_type=MESH,
        ).start()

    def begin(q):
        to_ring(z, q, 0, 0)
        to_ring(z, q, 1, 0)
        to_sibling(z, q, 0)

    def ring(q, step):
        for way in range(2):
            if step == 4 and way != q % 2:
                continue
            k = (8 - step) if way == 0 else step
            zo = lax.rem(z + k, 8)
            pending(xall.at[zo, c, q], recv_z.at[q, way, step - 1]).wait()
            if step < 3 or (step == 3 and way == q % 2):
                to_ring(zo, q, way, step)
            to_sibling(zo, q, k)

    def project(kind, q, group):
        f, half = q // 2, q % 2
        zs = [lax.rem(z + k, 8) for k in group]
        if kind == 0:
            for k, zo in zip(group, zs):
                pending(xall.at[zo, 1 - c, q], recv_d.at[q, k]).wait()

        pairs = [(zo, cc) for zo in zs for cc in range(2)]
        lhs = jnp.concatenate([xall[zo, cc, q, 0:512] for zo, cc in pairs], axis=1)
        if kind == 0:
            rhs = [wq_v[pl.ds(pl.multiple_of(zo * 512 + cc * 256 + f * 128, 128), 128)] for zo, cc in pairs]
        else:
            rhs = [wk[zo * 4 + cc * 2 + f] for zo, cc in pairs]
        got = jnp.dot(lhs, jnp.concatenate(rhs, axis=0), preferred_element_type=F32)
        at = pl.ds(half * 512, 512)
        if f == 0 and group is NEAR:
            acc[kind, at] = got
        else:
            acc[kind, at] += got

    def add_sums(ks):
        for half in range(2):
            total = jnp.zeros((8, 128), F32)
            for k in ks:
                for cc in range(2):
                    for f in range(2):
                        total += xall[lax.rem(z + k, 8), cc, 2 * f + half, 512:528].astype(F32)[0:8]
            sums[half] = total if sums[half] is None else sums[half] + total

    NEAR, MIDDLE, FAR, LAST = (0, 1, 7), (2, 6), (3, 5), (4,)
    sums = [None, None]
    distribute()
    for q in range(4):
        arrive(q)
        begin(q)
    lax.fori_loop(1, 8, send_wy, 0)
    for q in range(4):
        ring(q, 1)
    weights_x()
    take_wq.wait()
    ring(0, 2)
    project(0, 0, NEAR)
    ring(1, 2)
    project(0, 1, NEAR)
    weights_x2()
    ring(2, 2)
    project(0, 2, NEAR)
    ring(3, 2)
    weights_sibling()
    project(0, 3, NEAR)
    ring(0, 3)
    project(0, 0, MIDDLE)
    project(0, 1, MIDDLE)
    ring(1, 3)
    weights_ready()
    project(1, 0, NEAR)
    project(1, 1, NEAR)
    project(1, 2, NEAR)
    ring(2, 3)
    project(1, 3, NEAR)
    project(1, 0, MIDDLE)
    project(1, 1, MIDDLE)
    project(0, 2, MIDDLE)
    ring(3, 3)
    project(1, 2, MIDDLE)
    project(0, 3, MIDDLE)
    project(1, 3, MIDDLE)
    project(0, 0, FAR)
    project(1, 0, FAR)
    ring(0, 4)
    ring(1, 4)
    for q in range(1, 4):
        project(0, q, FAR)
        project(1, q, FAR)
    add_sums(NEAR + MIDDLE + FAR)
    for q in range(2):
        project(0, q, LAST)
        project(1, q, LAST)
    ring(2, 4)
    ring(3, 4)
    for q in range(2, 4):
        project(0, q, LAST)
        project(1, q, LAST)
    add_sums(LAST)
    sums = [part[0:4] + part[4:8] for part in sums]
    inverse = lax.rsqrt(jnp.concatenate(sums, axis=0) / D + 1e-05).T
    results = []
    for j in range(4):
        for half in range(2):
            start = half * 512 + j * 128
            factor = inverse[:, half * 4 + j : half * 4 + j + 1]
            for kind in range(2):
                scaled = (acc[kind, start : start + 128] * factor).astype(BF16)
                for e in range(2):
                    to = (2 * j + e) * 128 + half * 64
                    ready[to : to + 64, kind * 256 : kind * 256 + 256] = scaled[e * 64 : e * 64 + 64]
        at = pl.ds(256 * j, 256)
        result = pltpu.make_async_copy(ready.at[at], out.at[at], out_sem.at[j])
        result.start()
        results.append(result)

    pending(gathered.at[pl.ds(0, 248)], send_a).wait()
    pending(gathered.at[pl.ds(0, 248)], send_b).wait()
    pending(xall.at[pl.ds(0, 7), 0], send_z).wait()
    pending(xall.at[:, 0], send_d).wait()
    pending(wk.at[pl.ds(0, 7), half_rows], send_w.at[0]).wait()
    pending(wk.at[pl.ds(0, 24), half_rows], send_w.at[1]).wait()
    pending(wk.at[:, half_rows], send_w.at[2]).wait()
    for result in results:
        result.wait()


def attend_kernel(qkv, seg, out, held, buf, take_sem, sems):
    takes = []
    for i in range(4):
        at = pl.ds(256 * i, 256)
        take = pltpu.make_async_copy(qkv.at[at], held.at[at], take_sem.at[i])
        take.start()
        takes.append(take)
    docs = seg[...].astype(F32)
    columns = jnp.concatenate([docs[:, r * 128 : r * 128 + 128] for r in range(8)], axis=0).T
    copies = []
    for i in range(4):
        start, begin = 256 * i, max(0, 256 * i - 256)
        width = start + 256 - begin
        qdoc = jnp.concatenate([columns[:, 2 * i : 2 * i + 1], columns[:, 2 * i + 1 : 2 * i + 2]], axis=0)
        row = lax.broadcasted_iota(I32, (256, width), 0)
        col = lax.broadcasted_iota(I32, (256, width), 1)
        allowed = (qdoc == docs[:, begin : begin + width]) & (col <= row + (start - begin))
        takes[i].wait()
        keys = held[begin : begin + width, 2 * HD : 3 * HD]
        values = held[begin : begin + width, 3 * HD : 4 * HD]
        for h in range(2):
            s = lax.dot_general(
                held[start : start + 256, h * HD : (h + 1) * HD], keys, (((1,), (1,)), ((), ())),
                preferred_element_type=F32,
            )
            masked = jnp.where(allowed, s, -1e30)
            top = jnp.max(masked, axis=-1, keepdims=True)
            e = jnp.exp2((masked - top) * (math.log2(math.e) / math.sqrt(HD)))
            part = jnp.dot(e.astype(BF16), values, preferred_element_type=F32)
            part = part * (1.0 / jnp.sum(e, axis=-1, keepdims=True))
            buf[start : start + 256, h * HD : (h + 1) * HD] = part.astype(BF16)
        at = pl.ds(start, 256)
        copy = pltpu.make_async_copy(buf.at[at], out.at[at], sems.at[i])
        copy.start()
        copies.append(copy)
    for copy in copies:
        copy.wait()


def on_device(blocks, seg_ids, dest, slot, norm_gain, w_query, w_keyval):
    dma = pltpu.SemaphoreType.DMA
    hbm = pl.BlockSpec(memory_space=pltpu.HBM)
    vmem = pl.BlockSpec(memory_space=pltpu.VMEM)
    qkv = pl.pallas_call(
        exchange_kernel,
        out_shape=jax.ShapeDtypeStruct((1024, 512), BF16),
        in_specs=[vmem, vmem, hbm, vmem, hbm, hbm],
        out_specs=hbm,
        scratch_shapes=[
            pltpu.VMEM((8, 16, 8, 256), BF16),
            pltpu.VMEM((256, 8, 128), BF16),
            pltpu.VMEM((256, 8, 128), BF16),
            pltpu.VMEM((4, 8, 8, 8, 128), BF16),
            pltpu.VMEM((8, 2, 4, ROWS, 128), BF16),
            pltpu.VMEM((32, 128, 256), BF16),
            pltpu.VMEM((4096, 256), BF16),
            pltpu.VMEM((2, 1024, 256), F32),
            pltpu.VMEM((1024, 512), BF16),
            pltpu.VMEM((1, 256), I32),
            pltpu.SMEM((1, 256), I32),
            dma, dma, dma, dma((4,)), dma,
            dma, dma((32,)), dma, dma((32,)), dma, dma((4, 2, 4)), dma, dma((4, 8)),
            dma((3,)), dma((8,)), dma((2, 2)), dma,
        ],
        compiler_params=pltpu.CompilerParams(
            collective_id=0, has_side_effects=True, vmem_limit_bytes=60 * 1024 * 1024
        ),
        name="exchange",
    )(
        dest.reshape(2, 128),
        slot.reshape(2, 128),
        blocks.reshape(8, 16, 8, 256),
        norm_gain,
        w_keyval,
        w_query,
    )
    return pl.pallas_call(
        attend_kernel,
        out_shape=jax.ShapeDtypeStruct((1024, 256), BF16),
        in_specs=[hbm, vmem],
        out_specs=hbm,
        scratch_shapes=[pltpu.VMEM((1024, 512), BF16), pltpu.VMEM((1024, 256), BF16), dma((4,)), dma((4,))],
        compiler_params=pltpu.CompilerParams(vmem_limit_bytes=60 * 1024 * 1024),
        name="attend",
    )(qkv, seg_ids)


def solution(mesh):
    return jax.shard_map(
        on_device,
        mesh=mesh,
        in_specs=(
            P("learner", None, "tensor"),
            P("learner", None),
            P(),
            P(),
            P("tensor"),
            P(None, "tensor"),
            P("learner", None),
        ),
        out_specs=P("learner", "tensor"),
        check_vma=False,
    )
```

```python
import math

import jax
import jax.numpy as jnp
from jax import lax
from jax.experimental import pallas as pl
from jax.experimental.pallas import tpu as pltpu
from jax.sharding import PartitionSpec as P

D = 4096
HD = 128
MESH = pl.DeviceIdType.MESH
F32 = jnp.float32
BF16 = jnp.bfloat16
I32 = jnp.int32
ROWS = 528


def exchange_kernel(
    dest, slot, blocks, gain, wkv, wq, out,
    own, gathered, sorted_, landed, xall, wk, wq_v, acc, ready, inv_v, inv,
    own_sem, wq_sem, inv_sem, out_sem, w_sem,
    send_a, recv_a, send_b, recv_b, send_z, recv_z, send_d, recv_d,
    send_w, recv_wy, recv_wx, recv_wd,
):
    l = lax.axis_index("learner")
    t = lax.axis_index("tensor")
    x, y = lax.div(l, 8), lax.rem(l, 8)
    z, c = lax.div(t, 2), lax.rem(t, 2)
    other = z * 2 + (1 - c)
    up = lax.rem(z + 1, 8) * 2 + c
    down = lax.rem(z + 7, 8) * 2 + c

    def outward(k, middle):
        return middle + lax.div(k + 1, 2) * (1 - 2 * lax.rem(k, 2))

    def at_offset(i):
        dx, dy = outward(lax.div(i, 8), 2), outward(lax.rem(i, 8), 4)
        return lax.rem(x + dx, 4) * 8 + lax.rem(y + dy, 8)

    def peer(i, q):
        return lax.rem(x + outward(lax.div(i, 2), 2), 4) * 8 + lax.rem(lax.div(y, 4) + lax.rem(i, 2), 2) * 4 + q

    def place(j):
        return lax.div(j, 8) * 2 + lax.div(lax.rem(j, 8), 4)

    def pending(ref, sem):
        return pltpu.make_async_copy(ref, ref, sem)

    own_q = lax.rem(y, 4)
    own_place = place(l)

    barrier = pltpu.get_barrier_semaphore()

    def greet(i, carry):
        pl.semaphore_signal(barrier, inc=1, device_id=(at_offset(i), t), device_id_type=MESH)
        return carry

    lax.fori_loop(0, 31, greet, 0)
    for who in (up, down, other):
        pl.semaphore_signal(barrier, inc=1, device_id=(l, who), device_id_type=MESH)

    take_own = pltpu.make_async_copy(blocks, own, own_sem)
    take_own.start()
    take_wq = pltpu.make_async_copy(wq, wq_v, wq_sem)
    take_wq.start()
    position = dest[...] * 8 + slot[...]
    column = jnp.concatenate([position] * 4, axis=0).T
    where_to = lax.broadcasted_iota(I32, (128, 256), 1)
    who_from = lax.broadcasted_iota(I32, (128, 256), 0)
    table = jnp.zeros((1, 256), I32)
    for k in range(2):
        hit = column[:, k : k + 1] == where_to
        found = jnp.max(jnp.where(hit, who_from + 128 * k, 0), axis=0, keepdims=True)
        table = jnp.maximum(table, found)
    inv_v[...] = table
    take_inv = pltpu.make_async_copy(inv_v, inv, inv_sem)
    take_inv.start()
    take_own.wait()
    pl.semaphore_wait(barrier, 34)

    def rows_of(j):
        return pl.ds(pl.multiple_of(j * 8, 8), 8)

    def scatter(q):
        def send(i, carry):
            j = peer(i, q)
            src = own.at[:, 8 * (q % 2) + place(j), :, pl.ds((q // 2) * 128, 128)]

            @pl.when(j != l)
            def _():
                pltpu.make_async_remote_copy(
                    src_ref=src,
                    dst_ref=gathered.at[rows_of(l)],
                    send_sem=send_a,
                    recv_sem=recv_a.at[l],
                    device_id=(j, t),
                    device_id_type=MESH,
                ).start()

            @pl.when(j == l)
            def _():
                for b in range(8):
                    gathered[l * 8 + b] = own[b, 8 * (q % 2) + place(j), :, (q // 2) * 128 : (q // 2) * 128 + 128]

            return carry

        lax.fori_loop(0, 8, send, 0)

    scatter(0)
    scatter(1)
    scatter(2)
    scatter(3)
    take_inv.wait()

    def await_a(i, carry):
        j = at_offset(i)
        pending(gathered.at[rows_of(j)], recv_a.at[j]).wait()
        return carry

    def sort(j, carry):
        for s in range(8):
            sorted_[j * 8 + s] = gathered[inv[0, j * 8 + s]]
        return carry

    def send_out(i, carry):
        j = at_offset(i)
        pltpu.make_async_remote_copy(
            src_ref=sorted_.at[rows_of(j)],
            dst_ref=landed.at[own_q, :, own_place],
            send_sem=send_b,
            recv_sem=recv_b.at[l],
            device_id=(j, t),
            device_id_type=MESH,
        ).start()
        return carry

    def distribute():
        lax.fori_loop(0, 31, await_a, 0)
        lax.fori_loop(0, 32, sort, 0)
        lax.fori_loop(0, 31, send_out, 0)
        for s in range(8):
            landed[own_q, s, own_place] = sorted_[l * 8 + s]

    half_rows = pl.ds(pl.multiple_of(c * 64, 64), 64)
    w_src = wkv.at[half_rows, pl.ds(pl.multiple_of(z * 256, 256), 256)]
    take_w = pltpu.make_async_copy(w_src, wk.at[l, half_rows], w_sem)
    take_w.start()

    def send_wy(i, carry):
        pltpu.make_async_remote_copy(
            src_ref=w_src,
            dst_ref=wk.at[l, half_rows],
            send_sem=send_w.at[0],
            recv_sem=recv_wy.at[y],
            device_id=(x * 8 + lax.rem(y + i, 8), t),
            device_id_type=MESH,
        ).start()
        return carry

    def weights_x():
        take_w.wait()

        def await_wy(i, carry):
            yy = lax.rem(y + i, 8)
            pending(wk.at[x * 8 + yy, half_rows], recv_wy.at[yy]).wait()
            return carry

        lax.fori_loop(1, 8, await_wy, 0)
        for way in range(2):
            to_column(x, 8, 0, way)

    def column(xx, first, count):
        return wk.at[pl.ds(pl.multiple_of(xx * 8 + first, 4), count), half_rows]

    def to_column(xx, count, first, way):
        ref = column(xx, first, count)
        pltpu.make_async_remote_copy(
            src_ref=ref,
            dst_ref=ref,
            send_sem=send_w.at[1],
            recv_sem=recv_wx.at[way, 0 if count == 8 else 1],
            device_id=(lax.rem(x + (1 if way == 0 else 3), 4) * 8 + y, t),
            device_id_type=MESH,
        ).start()

    def weights_x2():
        for way in range(2):
            xx = lax.rem(x + (3 if way == 0 else 1), 4)
            pending(column(xx, 0, 8), recv_wx.at[way, 0]).wait()
            to_column(xx, 4, 4 * way, way)

    def weights_sibling():
        xx = lax.rem(x + 2, 4)
        for way in range(2):
            pending(column(xx, 4 * way, 4), recv_wx.at[way, 1]).wait()
        mine = wk.at[:, half_rows]
        pltpu.make_async_remote_copy(
            src_ref=mine,
            dst_ref=mine,
            send_sem=send_w.at[2],
            recv_sem=recv_wd,
            device_id=(l, other),
            device_id_type=MESH,
        ).start()

    def weights_ready():
        pending(wk.at[:, pl.ds(pl.multiple_of((1 - c) * 64, 64), 64)], recv_wd).wait()

    row = lax.broadcasted_iota(I32, (8, 128), 0)

    def arrive(q):
        def await_b(i, carry):
            j = peer(i, q)

            @pl.when(j != l)
            def _():
                pending(landed.at[q, :, place(j)], recv_b.at[j]).wait()

            return carry

        lax.fori_loop(0, 8, await_b, 0)
        f = q // 2
        g = gain[f * 128 : (f + 1) * 128].astype(F32).reshape(1, 128)
        ones = jnp.ones((8, 128), BF16)
        dims = (((1,), (1,)), ((), ()))

        def scale(j, total):
            xv = landed[q, pl.ds(2 * j, 2)].astype(F32).reshape(128, 128)
            xall[z, c, q, pl.ds(pl.multiple_of(j * 128, 128), 128)] = (xv * g).astype(BF16)
            sq = xv * xv
            hi = sq.astype(BF16)
            lo = (sq - hi.astype(F32)).astype(BF16)
            sums = lax.dot_general(ones, hi, dims, preferred_element_type=F32)
            sums += lax.dot_general(ones, lo, dims, preferred_element_type=F32)
            return jnp.where(lax.rem(row, 4) == j, sums, total)

        total = lax.fori_loop(0, 4, scale, jnp.zeros((8, 128), F32))
        hi = total.astype(BF16).astype(F32)
        tile = jnp.where(row < 4, hi, total - hi)
        xall[z, c, q, 512:528] = jnp.concatenate([tile, jnp.zeros((8, 128), F32)], axis=0).astype(BF16)

    def to_ring(zo, q, way, step):
        pltpu.make_async_remote_copy(
            src_ref=xall.at[zo, c, q],
            dst_ref=xall.at[zo, c, q],
            send_sem=send_z,
            recv_sem=recv_z.at[q, way, step],
            device_id=(l, up if way == 0 else down),
            device_id_type=MESH,
        ).start()

    def to_sibling(zo, q, k):
        pltpu.make_async_remote_copy(
            src_ref=xall.at[zo, c, q],
            dst_ref=xall.at[zo, c, q],
            send_sem=send_d,
            recv_sem=recv_d.at[q, k],
            device_id=(l, other),
            device_id_type=MESH,
        ).start()

    def begin(q):
        to_ring(z, q, 0, 0)
        to_ring(z, q, 1, 0)
        to_sibling(z, q, 0)

    def ring(q, step):
        for way in range(2):
            if step == 4 and way != q % 2:
                continue
            k = (8 - step) if way == 0 else step
            zo = lax.rem(z + k, 8)
            pending(xall.at[zo, c, q], recv_z.at[q, way, step - 1]).wait()
            if step < 3 or (step == 3 and way == q % 2):
                to_ring(zo, q, way, step)
            to_sibling(zo, q, k)

    def project(kind, q, group):
        f, half = q // 2, q % 2
        zs = [lax.rem(z + k, 8) for k in group]
        if kind == 0:
            for k, zo in zip(group, zs):
                pending(xall.at[zo, 1 - c, q], recv_d.at[q, k]).wait()

        pairs = [(zo, cc) for zo in zs for cc in range(2)]
        lhs = jnp.concatenate([xall[zo, cc, q, 0:512] for zo, cc in pairs], axis=1)
        if kind == 0:
            rhs = [wq_v[pl.ds(pl.multiple_of(zo * 512 + cc * 256 + f * 128, 128), 128)] for zo, cc in pairs]
        else:
            rhs = [wk[zo * 4 + cc * 2 + f] for zo, cc in pairs]
        got = jnp.dot(lhs, jnp.concatenate(rhs, axis=0), preferred_element_type=F32)
        at = pl.ds(half * 512, 512)
        if f == 0 and group is NEAR:
            acc[kind, at] = got
        else:
            acc[kind, at] += got

    def add_sums(ks):
        for half in range(2):
            total = jnp.zeros((8, 128), F32)
            for k in ks:
                for cc in range(2):
                    for f in range(2):
                        total += xall[lax.rem(z + k, 8), cc, 2 * f + half, 512:528].astype(F32)[0:8]
            sums[half] = total if sums[half] is None else sums[half] + total

    NEAR, MIDDLE, FAR, LAST = (0, 1, 7), (2, 6), (3, 5), (4,)
    sums = [None, None]
    distribute()
    for q in range(4):
        arrive(q)
        begin(q)
    lax.fori_loop(1, 8, send_wy, 0)
    for q in range(4):
        ring(q, 1)
    weights_x()
    take_wq.wait()
    ring(0, 2)
    project(0, 0, NEAR)
    ring(1, 2)
    project(0, 1, NEAR)
    weights_x2()
    ring(2, 2)
    project(0, 2, NEAR)
    ring(3, 2)
    weights_sibling()
    project(0, 3, NEAR)
    ring(0, 3)
    project(0, 0, MIDDLE)
    project(0, 1, MIDDLE)
    ring(1, 3)
    weights_ready()
    project(1, 0, NEAR)
    project(1, 1, NEAR)
    project(1, 2, NEAR)
    ring(2, 3)
    project(1, 3, NEAR)
    project(1, 0, MIDDLE)
    project(1, 1, MIDDLE)
    project(0, 2, MIDDLE)
    ring(3, 3)
    project(1, 2, MIDDLE)
    project(0, 3, MIDDLE)
    project(1, 3, MIDDLE)
    project(0, 0, FAR)
    project(1, 0, FAR)
    ring(0, 4)
    ring(1, 4)
    for q in range(1, 4):
        project(0, q, FAR)
        project(1, q, FAR)
    add_sums(NEAR + MIDDLE + FAR)
    for q in range(2):
        project(0, q, LAST)
        project(1, q, LAST)
    ring(2, 4)
    ring(3, 4)
    for q in range(2, 4):
        project(0, q, LAST)
        project(1, q, LAST)
    add_sums(LAST)
    sums = [part[0:4] + part[4:8] for part in sums]
    inverse = lax.rsqrt(jnp.concatenate(sums, axis=0) / D + 1e-05).T
    results = []
    for j in range(4):
        for half in range(2):
            start = half * 512 + j * 128
            factor = inverse[:, half * 4 + j : half * 4 + j + 1]
            for kind in range(2):
                scaled = (acc[kind, start : start + 128] * factor).astype(BF16)
                for e in range(2):
                    to = (2 * j + e) * 128 + half * 64
                    ready[to : to + 64, kind * 256 : kind * 256 + 256] = scaled[e * 64 : e * 64 + 64]
        at = pl.ds(256 * j, 256)
        result = pltpu.make_async_copy(ready.at[at], out.at[at], out_sem.at[j])
        result.start()
        results.append(result)

    pending(gathered.at[pl.ds(0, 248)], send_a).wait()
    pending(gathered.at[pl.ds(0, 248)], send_b).wait()
    pending(xall.at[pl.ds(0, 7), 0], send_z).wait()
    pending(xall.at[:, 0], send_d).wait()
    pending(wk.at[pl.ds(0, 7), half_rows], send_w.at[0]).wait()
    pending(wk.at[pl.ds(0, 24), half_rows], send_w.at[1]).wait()
    pending(wk.at[:, half_rows], send_w.at[2]).wait()
    for result in results:
        result.wait()


def attend_kernel(qkv, seg, out, held, buf, take_sem, sems):
    take = pltpu.make_async_copy(qkv, held, take_sem)
    take.start()
    docs = seg[...].astype(F32)
    columns = jnp.concatenate([docs[:, r * 128 : r * 128 + 128] for r in range(8)], axis=0).T
    masks = []
    for i in range(4):
        start, begin = 256 * i, max(0, 256 * i - 256)
        width = start + 256 - begin
        qdoc = jnp.concatenate([columns[:, 2 * i : 2 * i + 1], columns[:, 2 * i + 1 : 2 * i + 2]], axis=0)
        row = lax.broadcasted_iota(I32, (256, width), 0)
        col = lax.broadcasted_iota(I32, (256, width), 1)
        masks.append((qdoc == docs[:, begin : begin + width]) & (col <= row + (start - begin)))
    take.wait()
    scores = []
    dims = (((1,), (1,)), ((), ()))
    for i in range(4):
        start, begin = 256 * i, max(0, 256 * i - 256)
        width = start + 256 - begin
        keys = held[begin : begin + width, 2 * HD : 3 * HD]
        values = held[begin : begin + width, 3 * HD : 4 * HD]
        both = []
        for h in range(2):
            q = held[start : start + 256, h * HD : (h + 1) * HD]
            s = lax.dot_general(q, keys, dims, preferred_element_type=F32)
            both.append(s)
        scores.append(both)
    for i in range(4):
        start, begin = 256 * i, max(0, 256 * i - 256)
        width = start + 256 - begin
        values = held[begin : begin + width, 3 * HD : 4 * HD]
        for h in range(2):
            masked = jnp.where(masks[i], scores[i][h], -1e30)
            top = jnp.max(masked, axis=-1, keepdims=True)
            e = jnp.exp2((masked - top) * (math.log2(math.e) / math.sqrt(HD)))
            part = jnp.dot(e.astype(BF16), values, preferred_element_type=F32)
            part = part * (1.0 / jnp.sum(e, axis=-1, keepdims=True))
            buf[start : start + 256, h * HD : (h + 1) * HD] = part.astype(BF16)
    copy = pltpu.make_async_copy(buf, out, sems)
    copy.start()
    copy.wait()


def on_device(blocks, seg_ids, dest, slot, norm_gain, w_query, w_keyval):
    dma = pltpu.SemaphoreType.DMA
    hbm = pl.BlockSpec(memory_space=pltpu.HBM)
    vmem = pl.BlockSpec(memory_space=pltpu.VMEM)
    qkv = pl.pallas_call(
        exchange_kernel,
        out_shape=jax.ShapeDtypeStruct((1024, 512), BF16),
        in_specs=[vmem, vmem, hbm, vmem, hbm, hbm],
        out_specs=hbm,
        scratch_shapes=[
            pltpu.VMEM((8, 16, 8, 256), BF16),
            pltpu.VMEM((256, 8, 128), BF16),
            pltpu.VMEM((256, 8, 128), BF16),
            pltpu.VMEM((4, 8, 8, 8, 128), BF16),
            pltpu.VMEM((8, 2, 4, ROWS, 128), BF16),
            pltpu.VMEM((32, 128, 256), BF16),
            pltpu.VMEM((4096, 256), BF16),
            pltpu.VMEM((2, 1024, 256), F32),
            pltpu.VMEM((1024, 512), BF16),
            pltpu.VMEM((1, 256), I32),
            pltpu.SMEM((1, 256), I32),
            dma, dma, dma, dma((4,)), dma,
            dma, dma((32,)), dma, dma((32,)), dma, dma((4, 2, 4)), dma, dma((4, 8)),
            dma((3,)), dma((8,)), dma((2, 2)), dma,
        ],
        compiler_params=pltpu.CompilerParams(
            collective_id=0, has_side_effects=True, vmem_limit_bytes=60 * 1024 * 1024
        ),
        name="exchange",
    )(
        dest.reshape(2, 128),
        slot.reshape(2, 128),
        blocks.reshape(8, 16, 8, 256),
        norm_gain,
        w_keyval,
        w_query,
    )
    return pl.pallas_call(
        attend_kernel,
        out_shape=jax.ShapeDtypeStruct((1024, 256), BF16),
        in_specs=[hbm, vmem],
        out_specs=hbm,
        scratch_shapes=[pltpu.VMEM((1024, 512), BF16), pltpu.VMEM((1024, 256), BF16), dma, dma],
        compiler_params=pltpu.CompilerParams(vmem_limit_bytes=60 * 1024 * 1024),
        name="attend",
    )(qkv, seg_ids)


def solution(mesh):
    return jax.shard_map(
        on_device,
        mesh=mesh,
        in_specs=(
            P("learner", None, "tensor"),
            P("learner", None),
            P(),
            P(),
            P("tensor"),
            P(None, "tensor"),
            P("learner", None),
        ),
        out_specs=P("learner", "tensor"),
        check_vma=False,
    )
```

```python
import math

import jax
import jax.numpy as jnp
from jax import lax
from jax.experimental import pallas as pl
from jax.experimental.pallas import tpu as pltpu
from jax.sharding import PartitionSpec as P

D = 4096
HD = 128
MESH = pl.DeviceIdType.MESH
F32 = jnp.float32
BF16 = jnp.bfloat16
I32 = jnp.int32
ROWS = 528


def exchange_kernel(
    dest, slot, blocks, gain, wkv, wq, out,
    own, gathered, sorted_, landed, xall, wk, wq_v, acc, ready, inv_v, inv,
    own_sem, wq_sem, inv_sem, out_sem, w_sem,
    send_a, recv_a, send_b, recv_b, send_z, recv_z, send_d, recv_d,
    send_w, recv_wy, recv_wx, recv_wd,
):
    l = lax.axis_index("learner")
    t = lax.axis_index("tensor")
    x, y = lax.div(l, 8), lax.rem(l, 8)
    z, c = lax.div(t, 2), lax.rem(t, 2)
    other = z * 2 + (1 - c)
    up = lax.rem(z + 1, 8) * 2 + c
    down = lax.rem(z + 7, 8) * 2 + c

    def outward(k, middle):
        return middle + lax.div(k + 1, 2) * (1 - 2 * lax.rem(k, 2))

    def at_offset(i):
        dx, dy = outward(lax.div(i, 8), 2), outward(lax.rem(i, 8), 4)
        return lax.rem(x + dx, 4) * 8 + lax.rem(y + dy, 8)

    def peer(i, q):
        return lax.rem(x + outward(lax.div(i, 2), 2), 4) * 8 + lax.rem(lax.div(y, 4) + lax.rem(i, 2), 2) * 4 + q

    def place(j):
        return lax.div(j, 8) * 2 + lax.div(lax.rem(j, 8), 4)

    def pending(ref, sem):
        return pltpu.make_async_copy(ref, ref, sem)

    own_q = lax.rem(y, 4)
    own_place = place(l)

    barrier = pltpu.get_barrier_semaphore()

    def greet(i, carry):
        pl.semaphore_signal(barrier, inc=1, device_id=(at_offset(i), t), device_id_type=MESH)
        return carry

    lax.fori_loop(0, 31, greet, 0)
    for who in (up, down, other):
        pl.semaphore_signal(barrier, inc=1, device_id=(l, who), device_id_type=MESH)

    take_own = pltpu.make_async_copy(blocks, own, own_sem)
    take_own.start()
    take_wq = pltpu.make_async_copy(wq, wq_v, wq_sem)
    take_wq.start()
    position = dest[...] * 8 + slot[...]
    column = jnp.concatenate([position] * 4, axis=0).T
    where_to = lax.broadcasted_iota(I32, (128, 256), 1)
    who_from = lax.broadcasted_iota(I32, (128, 256), 0)
    table = jnp.zeros((1, 256), I32)
    for k in range(2):
        hit = column[:, k : k + 1] == where_to
        found = jnp.max(jnp.where(hit, who_from + 128 * k, 0), axis=0, keepdims=True)
        table = jnp.maximum(table, found)
    inv_v[...] = table
    take_inv = pltpu.make_async_copy(inv_v, inv, inv_sem)
    take_inv.start()
    take_own.wait()
    pl.semaphore_wait(barrier, 34)

    def rows_of(j):
        return pl.ds(pl.multiple_of(j * 8, 8), 8)

    def scatter(q):
        def send(i, carry):
            j = peer(i, q)
            src = own.at[:, 8 * (q % 2) + place(j), :, pl.ds((q // 2) * 128, 128)]

            @pl.when(j != l)
            def _():
                pltpu.make_async_remote_copy(
                    src_ref=src,
                    dst_ref=gathered.at[rows_of(l)],
                    send_sem=send_a,
                    recv_sem=recv_a.at[l],
                    device_id=(j, t),
                    device_id_type=MESH,
                ).start()

            @pl.when(j == l)
            def _():
                for b in range(8):
                    gathered[l * 8 + b] = own[b, 8 * (q % 2) + place(j), :, (q // 2) * 128 : (q // 2) * 128 + 128]

            return carry

        lax.fori_loop(0, 8, send, 0)

    scatter(0)
    scatter(1)
    scatter(2)
    scatter(3)
    take_inv.wait()

    def await_a(i, carry):
        j = at_offset(i)
        pending(gathered.at[rows_of(j)], recv_a.at[j]).wait()
        return carry

    def sort(j, carry):
        for s in range(8):
            sorted_[j * 8 + s] = gathered[inv[0, j * 8 + s]]
        return carry

    def send_out(i, carry):
        j = at_offset(i)
        pltpu.make_async_remote_copy(
            src_ref=sorted_.at[rows_of(j)],
            dst_ref=landed.at[own_q, :, own_place],
            send_sem=send_b,
            recv_sem=recv_b.at[l],
            device_id=(j, t),
            device_id_type=MESH,
        ).start()
        return carry

    def distribute():
        lax.fori_loop(0, 31, await_a, 0)
        lax.fori_loop(0, 32, sort, 0)
        lax.fori_loop(0, 31, send_out, 0)
        for s in range(8):
            landed[own_q, s, own_place] = sorted_[l * 8 + s]

    half_rows = pl.ds(pl.multiple_of(c * 64, 64), 64)
    w_src = wkv.at[half_rows, pl.ds(pl.multiple_of(z * 256, 256), 256)]
    take_w = pltpu.make_async_copy(w_src, wk.at[l, half_rows], w_sem)
    take_w.start()

    def send_wy(i, carry):
        pltpu.make_async_remote_copy(
            src_ref=w_src,
            dst_ref=wk.at[l, half_rows],
            send_sem=send_w.at[0],
            recv_sem=recv_wy.at[y],
            device_id=(x * 8 + lax.rem(y + i, 8), t),
            device_id_type=MESH,
        ).start()
        return carry

    def weights_x():
        take_w.wait()

        def await_wy(i, carry):
            yy = lax.rem(y + i, 8)
            pending(wk.at[x * 8 + yy, half_rows], recv_wy.at[yy]).wait()
            return carry

        lax.fori_loop(1, 8, await_wy, 0)
        for way in range(2):
            to_column(x, 8, 0, way)

    def column(xx, first, count):
        return wk.at[pl.ds(pl.multiple_of(xx * 8 + first, 4), count), half_rows]

    def to_column(xx, count, first, way):
        ref = column(xx, first, count)
        pltpu.make_async_remote_copy(
            src_ref=ref,
            dst_ref=ref,
            send_sem=send_w.at[1],
            recv_sem=recv_wx.at[way, 0 if count == 8 else 1],
            device_id=(lax.rem(x + (1 if way == 0 else 3), 4) * 8 + y, t),
            device_id_type=MESH,
        ).start()

    def weights_x2():
        for way in range(2):
            xx = lax.rem(x + (3 if way == 0 else 1), 4)
            pending(column(xx, 0, 8), recv_wx.at[way, 0]).wait()
            to_column(xx, 4, 4 * way, way)

    def weights_sibling():
        xx = lax.rem(x + 2, 4)
        for way in range(2):
            pending(column(xx, 4 * way, 4), recv_wx.at[way, 1]).wait()
        mine = wk.at[:, half_rows]
        pltpu.make_async_remote_copy(
            src_ref=mine,
            dst_ref=mine,
            send_sem=send_w.at[2],
            recv_sem=recv_wd,
            device_id=(l, other),
            device_id_type=MESH,
        ).start()

    def weights_ready():
        pending(wk.at[:, pl.ds(pl.multiple_of((1 - c) * 64, 64), 64)], recv_wd).wait()

    row = lax.broadcasted_iota(I32, (8, 128), 0)

    squares = {}

    def part(zo, cc, q):
        return xall.at[zo, cc, q, pl.ds(0, 512 if q < 2 else ROWS)]

    def arrive(q):
        def await_b(i, carry):
            j = peer(i, q)

            @pl.when(j != l)
            def _():
                pending(landed.at[q, :, place(j)], recv_b.at[j]).wait()

            return carry

        lax.fori_loop(0, 8, await_b, 0)
        f = q // 2
        g = gain[f * 128 : (f + 1) * 128].astype(F32).reshape(1, 128)
        ones = jnp.ones((8, 128), BF16)
        dims = (((1,), (1,)), ((), ()))

        def scale(j, total):
            xv = landed[q, pl.ds(2 * j, 2)].astype(F32).reshape(128, 128)
            xall[z, c, q, pl.ds(pl.multiple_of(j * 128, 128), 128)] = (xv * g).astype(BF16)
            sq = xv * xv
            hi = sq.astype(BF16)
            lo = (sq - hi.astype(F32)).astype(BF16)
            sums = lax.dot_general(ones, hi, dims, preferred_element_type=F32)
            sums += lax.dot_general(ones, lo, dims, preferred_element_type=F32)
            return jnp.where(lax.rem(row, 4) == j, sums, total)

        total = lax.fori_loop(0, 4, scale, jnp.zeros((8, 128), F32))
        if f == 0:
            squares[q] = total
            return
        total = total + squares[q - 2]
        hi = total.astype(BF16).astype(F32)
        tile = jnp.where(row < 4, hi, total - hi)
        xall[z, c, q, 512:528] = jnp.concatenate([tile, jnp.zeros((8, 128), F32)], axis=0).astype(BF16)

    def to_ring(zo, q, way, step):
        pltpu.make_async_remote_copy(
            src_ref=part(zo, c, q),
            dst_ref=part(zo, c, q),
            send_sem=send_z.at[q // 2],
            recv_sem=recv_z.at[q, way, step],
            device_id=(l, up if way == 0 else down),
            device_id_type=MESH,
        ).start()

    def to_sibling(zo, q, k):
        pltpu.make_async_remote_copy(
            src_ref=part(zo, c, q),
            dst_ref=part(zo, c, q),
            send_sem=send_d.at[q // 2],
            recv_sem=recv_d.at[q, k],
            device_id=(l, other),
            device_id_type=MESH,
        ).start()

    def begin(q):
        to_ring(z, q, 0, 0)
        to_ring(z, q, 1, 0)
        to_sibling(z, q, 0)

    def ring(q, step):
        for way in range(2):
            if step == 4 and way != q % 2:
                continue
            k = (8 - step) if way == 0 else step
            zo = lax.rem(z + k, 8)
            pending(part(zo, c, q), recv_z.at[q, way, step - 1]).wait()
            if step < 3 or (step == 3 and way == q % 2):
                to_ring(zo, q, way, step)
            to_sibling(zo, q, k)

    def project(kind, q, group):
        f, half = q // 2, q % 2
        zs = [lax.rem(z + k, 8) for k in group]
        if kind == 0:
            for k, zo in zip(group, zs):
                pending(part(zo, 1 - c, q), recv_d.at[q, k]).wait()

        pairs = [(zo, cc) for zo in zs for cc in range(2)]
        lhs = jnp.concatenate([xall[zo, cc, q, 0:512] for zo, cc in pairs], axis=1)
        if kind == 0:
            rhs = [wq_v[pl.ds(pl.multiple_of(zo * 512 + cc * 256 + f * 128, 128), 128)] for zo, cc in pairs]
        else:
            rhs = [wk[zo * 4 + cc * 2 + f] for zo, cc in pairs]
        got = jnp.dot(lhs, jnp.concatenate(rhs, axis=0), preferred_element_type=F32)
        at = pl.ds(half * 512, 512)
        if f == 0 and group is NEAR:
            acc[kind, at] = got
        else:
            acc[kind, at] += got

    def add_sums(ks):
        for half in range(2):
            total = jnp.zeros((8, 128), F32)
            for k in ks:
                for cc in range(2):
                    total += xall[lax.rem(z + k, 8), cc, 2 + half, 512:528].astype(F32)[0:8]
            sums[half] = total if sums[half] is None else sums[half] + total

    NEAR, MIDDLE, FAR, LAST = (0, 1, 7), (2, 6), (3, 5), (4,)
    sums = [None, None]
    distribute()
    for q in range(4):
        arrive(q)
        begin(q)
    lax.fori_loop(1, 8, send_wy, 0)
    for q in range(4):
        ring(q, 1)
    weights_x()
    take_wq.wait()
    ring(0, 2)
    project(0, 0, NEAR)
    ring(1, 2)
    project(0, 1, NEAR)
    weights_x2()
    ring(2, 2)
    project(0, 2, NEAR)
    ring(3, 2)
    weights_sibling()
    project(0, 3, NEAR)
    ring(0, 3)
    project(0, 0, MIDDLE)
    project(0, 1, MIDDLE)
    ring(1, 3)
    weights_ready()
    project(1, 0, NEAR)
    project(1, 1, NEAR)
    project(1, 2, NEAR)
    ring(2, 3)
    project(1, 3, NEAR)
    project(1, 0, MIDDLE)
    project(1, 1, MIDDLE)
    project(0, 2, MIDDLE)
    ring(3, 3)
    project(1, 2, MIDDLE)
    project(0, 3, MIDDLE)
    project(1, 3, MIDDLE)
    project(0, 0, FAR)
    project(1, 0, FAR)
    ring(0, 4)
    ring(1, 4)
    for q in range(1, 4):
        project(0, q, FAR)
        project(1, q, FAR)
    add_sums(NEAR + MIDDLE + FAR)
    for q in range(2):
        project(0, q, LAST)
        project(1, q, LAST)
    ring(2, 4)
    ring(3, 4)
    for q in range(2, 4):
        project(0, q, LAST)
        project(1, q, LAST)
    add_sums(LAST)
    sums = [part[0:4] + part[4:8] for part in sums]
    inverse = lax.rsqrt(jnp.concatenate(sums, axis=0) / D + 1e-05).T
    results = []
    for j in range(4):
        for half in range(2):
            start = half * 512 + j * 128
            factor = inverse[:, half * 4 + j : half * 4 + j + 1]
            for kind in range(2):
                scaled = (acc[kind, start : start + 128] * factor).astype(BF16)
                for e in range(2):
                    to = (2 * j + e) * 128 + half * 64
                    ready[to : to + 64, kind * 256 : kind * 256 + 256] = scaled[e * 64 : e * 64 + 64]
        at = pl.ds(256 * j, 256)
        result = pltpu.make_async_copy(ready.at[at], out.at[at], out_sem.at[j])
        result.start()
        results.append(result)

    pending(gathered.at[pl.ds(0, 248)], send_a).wait()
    pending(gathered.at[pl.ds(0, 248)], send_b).wait()
    for f, rows in enumerate((512, ROWS)):
        chunks = pl.ds(2 * f, 2)
        pending(xall.at[pl.ds(0, 7), 0, chunks, pl.ds(0, rows)], send_z.at[f]).wait()
        pending(xall.at[:, 0, chunks, pl.ds(0, rows)], send_d.at[f]).wait()
    pending(wk.at[pl.ds(0, 7), half_rows], send_w.at[0]).wait()
    pending(wk.at[pl.ds(0, 24), half_rows], send_w.at[1]).wait()
    pending(wk.at[:, half_rows], send_w.at[2]).wait()
    for result in results:
        result.wait()


def attend_kernel(qkv, seg, out, held, buf, take_sem, sems):
    take = pltpu.make_async_copy(qkv, held, take_sem)
    take.start()
    docs = seg[...].astype(F32)
    columns = jnp.concatenate([docs[:, r * 128 : r * 128 + 128] for r in range(8)], axis=0).T
    masks = []
    for i in range(4):
        start, begin = 256 * i, max(0, 256 * i - 256)
        width = start + 256 - begin
        qdoc = jnp.concatenate([columns[:, 2 * i : 2 * i + 1], columns[:, 2 * i + 1 : 2 * i + 2]], axis=0)
        row = lax.broadcasted_iota(I32, (256, width), 0)
        col = lax.broadcasted_iota(I32, (256, width), 1)
        masks.append((qdoc == docs[:, begin : begin + width]) & (col <= row + (start - begin)))
    take.wait()
    scores = []
    dims = (((1,), (1,)), ((), ()))
    for i in range(4):
        start, begin = 256 * i, max(0, 256 * i - 256)
        width = start + 256 - begin
        keys = held[begin : begin + width, 2 * HD : 3 * HD]
        values = held[begin : begin + width, 3 * HD : 4 * HD]
        both = []
        for h in range(2):
            q = held[start : start + 256, h * HD : (h + 1) * HD]
            s = lax.dot_general(q, keys, dims, preferred_element_type=F32)
            both.append(s)
        scores.append(both)
    for i in range(4):
        start, begin = 256 * i, max(0, 256 * i - 256)
        width = start + 256 - begin
        values = held[begin : begin + width, 3 * HD : 4 * HD]
        for h in range(2):
            masked = jnp.where(masks[i], scores[i][h], -1e30)
            top = jnp.max(masked, axis=-1, keepdims=True)
            e = jnp.exp2((masked - top) * (math.log2(math.e) / math.sqrt(HD)))
            part = jnp.dot(e.astype(BF16), values, preferred_element_type=F32)
            part = part * (1.0 / jnp.sum(e, axis=-1, keepdims=True))
            buf[start : start + 256, h * HD : (h + 1) * HD] = part.astype(BF16)
    copy = pltpu.make_async_copy(buf, out, sems)
    copy.start()
    copy.wait()


def on_device(blocks, seg_ids, dest, slot, norm_gain, w_query, w_keyval):
    dma = pltpu.SemaphoreType.DMA
    hbm = pl.BlockSpec(memory_space=pltpu.HBM)
    vmem = pl.BlockSpec(memory_space=pltpu.VMEM)
    qkv = pl.pallas_call(
        exchange_kernel,
        out_shape=jax.ShapeDtypeStruct((1024, 512), BF16),
        in_specs=[vmem, vmem, hbm, vmem, hbm, hbm],
        out_specs=hbm,
        scratch_shapes=[
            pltpu.VMEM((8, 16, 8, 256), BF16),
            pltpu.VMEM((256, 8, 128), BF16),
            pltpu.VMEM((256, 8, 128), BF16),
            pltpu.VMEM((4, 8, 8, 8, 128), BF16),
            pltpu.VMEM((8, 2, 4, ROWS, 128), BF16),
            pltpu.VMEM((32, 128, 256), BF16),
            pltpu.VMEM((4096, 256), BF16),
            pltpu.VMEM((2, 1024, 256), F32),
            pltpu.VMEM((1024, 512), BF16),
            pltpu.VMEM((1, 256), I32),
            pltpu.SMEM((1, 256), I32),
            dma, dma, dma, dma((4,)), dma,
            dma, dma((32,)), dma, dma((32,)), dma((2,)), dma((4, 2, 4)), dma((2,)), dma((4, 8)),
            dma((3,)), dma((8,)), dma((2, 2)), dma,
        ],
        compiler_params=pltpu.CompilerParams(
            collective_id=0, has_side_effects=True, vmem_limit_bytes=60 * 1024 * 1024
        ),
        name="exchange",
    )(
        dest.reshape(2, 128),
        slot.reshape(2, 128),
        blocks.reshape(8, 16, 8, 256),
        norm_gain,
        w_keyval,
        w_query,
    )
    return pl.pallas_call(
        attend_kernel,
        out_shape=jax.ShapeDtypeStruct((1024, 256), BF16),
        in_specs=[hbm, vmem],
        out_specs=hbm,
        scratch_shapes=[pltpu.VMEM((1024, 512), BF16), pltpu.VMEM((1024, 256), BF16), dma, dma],
        compiler_params=pltpu.CompilerParams(vmem_limit_bytes=60 * 1024 * 1024),
        name="attend",
    )(qkv, seg_ids)


def solution(mesh):
    return jax.shard_map(
        on_device,
        mesh=mesh,
        in_specs=(
            P("learner", None, "tensor"),
            P("learner", None),
            P(),
            P(),
            P("tensor"),
            P(None, "tensor"),
            P("learner", None),
        ),
        out_specs=P("learner", "tensor"),
        check_vma=False,
    )
```
